512 devices in a mesh: groups: 2 (over y), sample: 32 (over z), fsdp: 4 (over x), prompt: 2 (over core).
Axes of the slice: x: 4, y: 2, z: 32, core: 2. Of those that a mesh axis runs over, the one named last changes fastest.
The devices are a block of a 4x8x32 slice.
Arguments:
- queries: bfloat16 [4, 32, 512, 4096], P(('groups', 'prompt'), 'sample', 'fsdp'), parts along dimension 0, may hold values from -16 to 16
- completion_keys: bfloat16 [4, 32, 512, 512], P(('groups', 'prompt'), 'sample', 'fsdp'), parts along dimension 0, may hold values from -6 to 6
- completion_values: bfloat16 [4, 32, 512, 512], P(('groups', 'prompt'), 'sample', 'fsdp'), parts along dimension 0, may hold values from -6 to 6
- prompt_keys: bfloat16 [4, 128, 512], P(('groups', 'prompt'), ('sample', 'fsdp')), parts along dimension 0, may hold values from -6 to 6
- prompt_values: bfloat16 [4, 128, 512], P(('groups', 'prompt'), ('sample', 'fsdp')), parts along dimension 0, may hold values from -6 to 6
- output_grad: bfloat16 [4, 32, 512, 4096], P(('groups', 'prompt'), 'sample', 'fsdp'), parts along dimension 0, may hold values from -6 to 6
- lengths: int32 [4, 32], P(('groups', 'prompt'), 'sample'), parts along dimension 0, may hold values from 128 to 512
Outputs:
- attention_out: bfloat16 [4, 32, 512, 4096], P(('groups', 'prompt'), 'sample', 'fsdp'), parts along dimension 0
- query_grad: bfloat16 [4, 32, 512, 4096], P(('groups', 'prompt'), 'sample', 'fsdp'), parts along dimension 0
- completion_key_grad: float32 [4, 32, 512, 512], P(('groups', 'prompt'), 'sample', 'fsdp'), parts along dimension 0
- completion_value_grad: float32 [4, 32, 512, 512], P(('groups', 'prompt'), 'sample', 'fsdp'), parts along dimension 0
- shared_prompt_key_gradient: float32 [4, 128, 512], P(('groups', 'prompt'), ('sample', 'fsdp')), parts along dimension 0
- shared_prompt_value_gradient: float32 [4, 128, 512], P(('groups', 'prompt'), ('sample', 'fsdp')), parts along dimension 0
The draws below stay inside these ranges and needn't reach their ends.
There are 2 independent parts, one for each index of `groups`. The reference program is written for one: setup_inputs(seed, part) draws one part's arguments, and reference() takes and returns one part's arrays. A program takes and returns all parts, laid end to end along the dimension named above; each array names one. Nothing has to cross between parts.
All inputs are finite; a program needn't handle non-finite values.
Results may differ from the reference program's by a relative error of at most 0.02.
Values may be sent and summed in bfloat16 or wider, within the bound.
A program may use at most 128 MiB of HBM per device.

```python
import jax
import jax.numpy as jnp
from jax import lax

HEADS = 32
KV_HEADS = 4
HEAD_DIM = 128
COMP_LEN = 512
PROMPT_LEN = 128
COMPLETIONS = 32


def draw_prompt_keys(key, part):
    noise_key = jax.random.fold_in(key, 31)
    drawn = jnp.clip(jax.random.normal(noise_key, (2, PROMPT_LEN, KV_HEADS * HEAD_DIM), jnp.float32), -6.0, 6.0)
    return drawn.astype(jnp.bfloat16)


def draw_queries(key, part):
    noise_key = jax.random.fold_in(key, 47)
    shape = (2, COMPLETIONS, COMP_LEN, HEADS * HEAD_DIM)
    drawn = jnp.clip(jax.random.normal(noise_key, shape, jnp.float32), -6.0, 6.0)
    return drawn.astype(jnp.bfloat16)


def with_ends(values, stream_key, least, largest):
    dims = values.shape
    index_at = [jax.random.randint(jax.random.fold_in(stream_key, axis), (), 0, dims[axis]) for axis in range(len(dims))]
    values = values.at[tuple(index_at)].set(least)
    longest = dims.index(max(dims))
    index_at[longest] = (index_at[longest] + 1) % dims[longest]
    return values.at[tuple(index_at)].set(largest)


def steps_of(key, dims, shards, least, high):
    factor_of = 1.0
    for dim, shards_of in shards:
        heights = jax.random.uniform(jax.random.fold_in(jax.random.fold_in(key, 6), dim), (shards_of,), jnp.float32, least / len(shards), high / len(shards))
        factor_of = factor_of * jnp.repeat(jnp.exp(heights), dims[dim] // shards_of).reshape((-1,) + (1,) * (len(dims) - 1 - dim))
    return factor_of


def scatter_about(stream_key, extent, width, limit, cuts=(), kind=jnp.bfloat16):
    array = jax.random.normal(stream_key, extent, jnp.float32) * width
    if len(cuts) > 0:
        array = steps_of(stream_key, extent, cuts, -0.22, 0.18) * array
    return jnp.clip(array, min=-limit, max=limit).astype(kind)


def setup_inputs(seed: int = 0, part: int = 0) -> dict:
    arg_keys = jax.random.split(jax.random.key(seed), 8)
    part_splits = jax.random.split(jax.random.fold_in(arg_keys[7], part), 8)
    return {
        "queries": draw_queries(jax.random.fold_in(jax.random.fold_in(arg_keys[7], part), 71), part),
        "completion_keys": scatter_about(part_splits[1], (2, COMPLETIONS, COMP_LEN, KV_HEADS * HEAD_DIM), 1.0, 6.0, ((0, 2), (1, 32), (2, 4))),
        "completion_values": scatter_about(part_splits[2], (2, COMPLETIONS, COMP_LEN, KV_HEADS * HEAD_DIM), 1.0, 6.0, ((0, 2), (1, 32), (2, 4))),
        "prompt_keys": draw_prompt_keys(jax.random.fold_in(jax.random.fold_in(arg_keys[7], part), 71), part),
        "prompt_values": scatter_about(part_splits[4], (2, PROMPT_LEN, KV_HEADS * HEAD_DIM), 1.0, 6.0, ((0, 2), (1, 128))),
        "output_grad": scatter_about(part_splits[5], (2, COMPLETIONS, COMP_LEN, HEADS * HEAD_DIM), 1.0, 6.0, ((0, 2), (1, 32), (2, 4))),
        "lengths": with_ends(jax.random.randint(part_splits[6], (2, COMPLETIONS), COMP_LEN // 4, COMP_LEN + 1), jax.random.fold_in(part_splits[6], 1), COMP_LEN // 4, COMP_LEN).astype(jnp.int32),
    }


def attend(query_rows, grad_input, length, prompt_keys, prompt_values, own_keys, own_values):
    prompt_span = prompt_keys.shape[0]
    comp_span = query_rows.shape[0]
    group_share = HEADS // KV_HEADS
    softmax_scale = HEAD_DIM ** -0.5
    key_data = jnp.concatenate([prompt_keys, own_keys], 0).reshape(-1, KV_HEADS, HEAD_DIM).astype(jnp.float32)
    value_data = jnp.concatenate([prompt_values, own_values], 0).reshape(-1, KV_HEADS, HEAD_DIM).astype(jnp.float32)
    query_data = query_rows.reshape(comp_span, KV_HEADS, group_share, HEAD_DIM).astype(jnp.float32)
    token_pos = jnp.arange(comp_span, dtype=jnp.int32)
    key_pos = jnp.arange(prompt_span + comp_span, dtype=jnp.int32)
    visible = (key_pos[None, :] < prompt_span) | (key_pos[None, :] - prompt_span <= token_pos[:, None])
    scores = jnp.einsum("tgrd,jgd->grtj", query_data, key_data) * softmax_scale
    scores = jnp.where(visible[None, None], scores, -jnp.inf)
    maximum = jnp.max(scores, axis=-1, keepdims=True)
    exponent = jnp.exp(scores - maximum)
    attention = exponent / jnp.sum(exponent, axis=-1, keepdims=True)
    attention_half = lax.optimization_barrier(attention.astype(jnp.bfloat16)).astype(jnp.float32)
    blended_output = jnp.einsum("grtj,jgd->tgrd", attention_half, value_data).astype(jnp.bfloat16)
    token_weight = jnp.where(token_pos < length, jnp.float32(comp_span) / length.astype(jnp.float32), jnp.float32(0.0))
    gradient_row_slice = (grad_input.astype(jnp.float32) * token_weight[:, None]).astype(jnp.bfloat16)
    gradient_tensor = lax.optimization_barrier(gradient_row_slice).astype(jnp.float32).reshape(comp_span, KV_HEADS, group_share, HEAD_DIM)
    row_inner_product = jnp.einsum("keqf,keqf->eqk", gradient_tensor, blended_output.astype(jnp.float32))
    prob_grad = jnp.einsum("tgrd,jgd->grtj", gradient_tensor, value_data)
    score_grad = (attention * (prob_grad - row_inner_product[..., None])).astype(jnp.bfloat16)
    score_grad = lax.optimization_barrier(score_grad).astype(jnp.float32)
    query_grad = (jnp.einsum("grtj,jgd->tgrd", score_grad, key_data) * softmax_scale).astype(jnp.bfloat16)
    key_grad = jnp.einsum("grtj,tgrd->jgd", score_grad, query_data) * softmax_scale
    value_grad = jnp.einsum("grtj,tgrd->jgd", attention_half, gradient_tensor)
    total = prompt_span + comp_span
    return (blended_output.reshape(comp_span, HEADS * HEAD_DIM), query_grad.reshape(comp_span, HEADS * HEAD_DIM),
            key_grad.reshape(total, KV_HEADS * HEAD_DIM), value_grad.reshape(total, KV_HEADS * HEAD_DIM))


def reference(queries, completion_keys, completion_values, prompt_keys, prompt_values, output_grad, lengths):
    mixed_all, query_all, own_key_all, own_value_all, prompt_key_all, prompt_value_all = [], [], [], [], [], []
    for prompt_index in range(2):
        def per_completion(items):
            return attend(items[0], items[1], items[2], prompt_keys[prompt_index], prompt_values[prompt_index], items[3], items[4])

        results = lax.map(per_completion, (queries[prompt_index], output_grad[prompt_index], lengths[prompt_index],
                                           completion_keys[prompt_index], completion_values[prompt_index]))
        mixed_all.append(results[0])
        query_all.append(results[1])
        own_key_all.append(results[2][:, PROMPT_LEN:])
        own_value_all.append(results[3][:, PROMPT_LEN:])
        prompt_key_all.append(jnp.sum(results[2][:, :PROMPT_LEN], axis=0))
        prompt_value_all.append(jnp.sum(results[3][:, :PROMPT_LEN], axis=0))
    return (jnp.stack(mixed_all), jnp.stack(query_all), jnp.stack(own_key_all), jnp.stack(own_value_all),
            jnp.stack(prompt_key_all), jnp.stack(prompt_value_all))
```

```python
import functools
import math

import jax
import jax.numpy as jnp
from jax import lax
from jax.experimental import pallas as pl
from jax.experimental.pallas import tpu as pltpu
from jax.sharding import PartitionSpec as P

HEAD_DIM = 128
TILE = 256
MESH = pl.DeviceIdType.MESH
F32 = jnp.float32
BF16 = jnp.bfloat16
NT = (((1,), (1,)), ((), ()))
NN = (((1,), (0,)), ((), ()))


def dot(a, b, dims=NN):
    return lax.dot_general(a, b, dims, preferred_element_type=F32)


def kernel(
    nz,
    nx,
    queries,
    comp_k,
    comp_v,
    prompt_k,
    prompt_v,
    out_grad,
    lengths,
    out,
    query_grad,
    comp_k_grad,
    comp_v_grad,
    prompt_k_grad,
    prompt_v_grad,
    q_s,
    g_s,
    kv,
    kvt,
    rows,
    rows32,
    e_s,
    dp_s,
    o_s,
    dq_s,
    stat,
    blockmax,
    p_half,
    ds_half,
    o_half,
    dq_half,
    csend,
    crecv,
    cown,
    cstage,
    xsend,
    xown,
    xrecv,
    zf,
    zsend,
    zrecv,
    pstage,
    in_sem,
    kvin_sem,
    out_sem,
    gout_sem,
    r1_send,
    r1_recv,
    r2_send,
    r2_recv,
    rx_send,
    rx_recv,
    kv_send,
    kv_recv,
    x_send,
    x_recv,
    z_send,
    z_recv,
    c_send,
    c_recv,
):
    z = lax.axis_index("sample")
    x = lax.axis_index("fsdp")
    count = comp_k.shape[2]
    groups = comp_k.shape[3] // HEAD_DIM
    heads = queries.shape[3] // HEAD_DIM
    share = heads // groups
    wide = share * count
    reach = nz // 4
    scale = HEAD_DIM**-0.5
    fold = scale * math.log2(math.e)
    last = nx
    key_count = nz * nx

    def at_z(d):
        return {"sample": lax.rem(z + (d + nz) % nz, nz)}

    def at_x(d):
        return {"fsdp": lax.rem(x + d, nx)}

    def remote(src, dst, send, recv, to):
        return pltpu.make_async_remote_copy(
            src_ref=src, dst_ref=dst, send_sem=send, recv_sem=recv, device_id=to, device_id_type=MESH
        )

    own_kv = [
        pltpu.make_async_copy(comp_k.at[0, 0], kv.at[x, 0], kvin_sem.at[0]),
        pltpu.make_async_copy(comp_v.at[0, 0], kv.at[x, 1], kvin_sem.at[1]),
    ]
    for c in own_kv:
        c.start()

    @pl.loop(0, groups)
    def _(g):
        for h in range(share):
            head = g * share + h
            cols = pl.ds(pl.multiple_of(head * HEAD_DIM, HEAD_DIM), HEAD_DIM)
            dst = pl.ds(pl.multiple_of(head * count, count), count)
            pltpu.make_async_copy(queries.at[0, 0, :, cols], q_s.at[dst], in_sem.at[0, g]).start()
            pltpu.make_async_copy(out_grad.at[0, 0, :, cols], g_s.at[dst], in_sem.at[1, g]).start()

    for k, ref in enumerate((prompt_k, prompt_v)):
        row = ref[0].astype(F32)
        for g in range(groups):
            pstage[k * groups + g : k * groups + g + 1, :] = row[:, g * HEAD_DIM : (g + 1) * HEAD_DIM]
    rows[0, 0] = pstage[...].astype(BF16)

    barrier = pltpu.get_barrier_semaphore()
    near = [d for d in range(1, reach + 1)] + [-d for d in range(1, reach + 1)]
    for d in near:
        pl.semaphore_signal(barrier, inc=1, device_id=at_z(d), device_id_type=MESH)
    for d in range(1, nx):
        pl.semaphore_signal(barrier, inc=1, device_id=at_x(d), device_id_type=MESH)

    def turn(b):
        for part in range(2):
            for g in range(groups):
                cols = slice(g * HEAD_DIM, (g + 1) * HEAD_DIM)
                kvt[b, part, cols, :] = kv[b, part, :, cols].astype(F32).T.astype(BF16)

    def forward(b, g, first):
        cols = pl.ds(pl.multiple_of(g * HEAD_DIM, HEAD_DIM), HEAD_DIM)
        keys = kv[b, 0, :, cols]
        values = kv[b, 1, :, cols]
        values_t = kvt[b, 1, cols, :]
        slot = g * (nx + 1) + b
        for t in range(wide // TILE):
            at = slice(t * TILE, (t + 1) * TILE)
            src = pl.ds(pl.multiple_of(g * wide + t * TILE, TILE), TILE)
            s = dot(keys, q_s[src, :], NT)
            if first:
                key = lax.broadcasted_iota(jnp.int32, s.shape, 0)
                token = lax.broadcasted_iota(jnp.int32, s.shape, 1) % count
                s = jnp.where(key <= token, s, -1e30)
            top = jnp.max(s, axis=0, keepdims=True)
            if not first:
                before = stat[g, 0:1, at]
                top = jnp.maximum(top, before)
            e = jnp.exp2((s - top) * fold)
            total = jnp.sum(e, axis=0, keepdims=True)
            dp = dot(values, g_s[src, :], NT)
            mean = jnp.sum(e * dp, axis=0, keepdims=True)
            o = dot(values_t, e.astype(BF16))
            if not first:
                old = jnp.exp2((before - top) * fold)
                total += old * stat[g, 1:2, at]
                mean += old * stat[g, 2:3, at]
                o += old * o_s[g, :, at]
            stat[g, 0:1, at] = top
            stat[g, 1:2, at] = total
            stat[g, 2:3, at] = mean
            o_s[g, :, at] = o
            e_s[slot, :, at] = e
            dp_s[slot, :, at] = dp
            blockmax[slot, 0:1, at] = top

    def backward(b, g, first):
        cols = pl.ds(pl.multiple_of(g * HEAD_DIM, HEAD_DIM), HEAD_DIM)
        keys_t = kvt[b, 0, cols, :]
        slot = g * (nx + 1) + b
        for t in range(wide // TILE):
            at = slice(t * TILE, (t + 1) * TILE)
            factor = jnp.exp2((blockmax[slot, 0:1, at] - stat[g, 0:1, at]) * fold) * stat[g, 1:2, at]
            p = e_s[slot, :, at] * factor
            ds = (p * (dp_s[slot, :, at] - stat[g, 2:3, at])).astype(BF16)
            p_half[:, at] = p.astype(BF16)
            ds_half[:, at] = ds
            dq = dot(keys_t, ds)
            if first:
                dq_s[g, :, at] = dq
            else:
                dq_s[g, :, at] += dq
        src = pl.ds(pl.multiple_of(g * wide, wide), wide)
        return dot(ds_half[...], q_s[src, :]) * scale, dot(p_half[...], g_s[src, :])

    def flush(source, staged, target, g, sem):
        for t in range(wide // TILE):
            at = slice(t * TILE, (t + 1) * TILE)
            dst = pl.ds(pl.multiple_of(g * wide + t * TILE, TILE), TILE)
            staged[dst, :] = source(at).T.astype(BF16)
        for h in range(share):
            head = g * share + h
            cols = pl.ds(pl.multiple_of(head * HEAD_DIM, HEAD_DIM), HEAD_DIM)
            src = pl.ds(pl.multiple_of(head * count, count), count)
            pltpu.make_async_copy(staged.at[src], target.at[0, 0, :, cols], sem).start()

    for c in own_kv:
        c.wait()
    turn(x)
    token = lax.broadcasted_iota(jnp.int32, (count, HEAD_DIM), 0) + x * count
    length = jnp.full((count, HEAD_DIM), lengths[0, 0], jnp.int32)
    weight = jnp.where(token < length, F32(count * nx) / length.astype(F32), 0.0)

    @pl.loop(0, groups)
    def _(g):
        src = pl.ds(pl.multiple_of(g * wide, wide), wide)
        pltpu.make_async_copy(q_s.at[src], q_s.at[src], in_sem.at[0, g]).wait()
        pltpu.make_async_copy(g_s.at[src], g_s.at[src], in_sem.at[1, g]).wait()
        for h in range(share):
            at = pl.ds(pl.multiple_of((g * share + h) * count, count), count)
            g_s[at, :] = (g_s[at, :].astype(F32) * weight).astype(BF16)
        forward(x, g, True)

    pl.semaphore_wait(barrier, len(near) + nx - 1)

    first_leg = {
        d: remote(
            rows.at[0, 0], rows.at[0, (nz - d) % nz], r1_send.at[n], r1_recv.at[n], at_z(d)
        )
        for n, d in enumerate(near)
    }
    for d in sorted(near, key=abs, reverse=True):
        first_leg[d].start()

    def kv_copy(d):
        return remote(kv.at[x], kv.at[x], kv_send.at[d - 1], kv_recv.at[d - 1], at_x(d))

    for d in range(1, nx):

        @pl.when(x + d < nx)
        def _(d=d):
            kv_copy(d).start()

    second_leg = []
    for e in range(1, reach + 1):
        first_leg[-e].wait_recv()
        c = remote(
            rows.at[0, e], rows.at[0, reach + e], r2_send.at[0, e - 1], r2_recv.at[0, e - 1], at_z(-reach)
        )
        c.start()
        second_leg.append(c)
        first_leg[e].wait_recv()
        if e < reach:
            c = remote(
                rows.at[0, nz - e],
                rows.at[0, nz - reach - e],
                r2_send.at[1, e - 1],
                r2_recv.at[1, e - 1],
                at_z(reach),
            )
            c.start()
            second_leg.append(c)

    def to_columns(part, begin, end):
        return [
            remote(
                rows.at[0, begin:end],
                rows.at[nx - d, begin:end],
                rx_send.at[part, d - 1],
                rx_recv.at[part, d - 1],
                at_x(d),
            )
            for d in range(1, nx)
        ]

    column_legs = to_columns(0, 0, reach + 1) + to_columns(1, nz - reach, nz)
    for c in column_legs:
        c.start()

    @pl.loop(0, x)
    def _(n):
        d = n + 1
        b = x - d
        remote(kv.at[b], kv.at[b], kv_send.at[n], kv_recv.at[n], at_x(1)).wait_recv()
        turn(b)

        @pl.loop(0, groups)
        def _(g):
            forward(b, g, False)

    for c in second_leg:
        c.wait_recv()
    final_legs = to_columns(2, reach + 1, nz - reach)
    for c in final_legs:
        c.start()
    column_legs += final_legs
    for c in column_legs:
        c.wait_recv()

    rows32[...] = rows[...].reshape(key_count, 2 * groups, HEAD_DIM).astype(F32)
    for part in range(2):
        for g in range(groups):
            cols = slice(g * HEAD_DIM, (g + 1) * HEAD_DIM)
            block = rows32[:, part * groups + g, :]
            kv[last, part, :, cols] = block.astype(BF16)
            kvt[last, part, cols, :] = block.T.astype(BF16)

    def x_copy(g, d):
        return remote(
            xsend.at[g, d], xrecv.at[g, nx - d], x_send.at[g, d - 1], x_recv.at[g, d - 1], at_x(d)
        )

    @pl.loop(0, groups)
    def _(g):
        forward(last, g, False)
        inverse = 1.0 / stat[g, 1:2, :]
        stat[g, 1:2, :] = inverse
        stat[g, 2:3, :] = stat[g, 2:3, :] * inverse
        both = backward(last, g, True)
        for part in range(2):
            xown[g, part] = both[part][:nz]
            for d in range(1, nx):
                xsend[g, d, part] = both[part][d * nz : (d + 1) * nz].astype(BF16)
        for d in range(1, nx):
            x_copy(g, d).start()
        flush(lambda at: o_s[g, :, at] * stat[g, 1:2, at], o_half, out, g, out_sem.at[0])

    def c_copy(b, g, d):
        return remote(
            csend.at[b, g], crecv.at[d - 1, g], c_send.at[b, g], c_recv.at[d - 1, g], {"fsdp": b}
        )

    def completion_backward(b):
        @pl.loop(0, groups)
        def _(g):
            both = backward(b, g, False)

            @pl.when(b < x)
            def _():
                for part in range(2):
                    csend[b, g, part] = both[part].astype(BF16)
                c_copy(b, g, x - b).start()

            @pl.when(b == x)
            def _():
                for part in range(2):
                    cown[g, part] = both[part]

    completion_backward(0)

    for g in range(groups):
        for d in range(1, nx):
            x_copy(g, d).wait_recv()
    for g in range(groups):
        for part in range(2):
            total = xown[g, part]
            for d in range(1, nx):
                total += xrecv[g, d, part].astype(F32)
            zf[:, part * groups + g, :] = total
    zsend[...] = zf[...].astype(BF16)

    def z_copy(s):
        return remote(zsend.at[s], zrecv.at[nz - s], z_send, z_recv, at_z(s))

    for s in sorted(range(1, nz), key=lambda s: min(s, nz - s), reverse=True):
        z_copy(s).start()

    @pl.loop(1, x + 1)
    def _(b):
        completion_backward(b)

    @pl.loop(0, groups)
    def _(g):
        flush(lambda at: dq_s[g, :, at] * scale, dq_half, query_grad, g, out_sem.at[1])

    for d in range(1, nx):

        @pl.when(x + d < nx)
        def _(d=d):
            for g in range(groups):
                remote(
                    csend.at[0, g], crecv.at[d - 1, g], c_send.at[0, g], c_recv.at[d - 1, g], at_x(d)
                ).wait_recv()
                for part in range(2):
                    cown[g, part] += crecv[d - 1, g, part].astype(F32)

    for part in range(2):
        for g in range(groups):
            cstage[part, :, g * HEAD_DIM : (g + 1) * HEAD_DIM] = cown[g, part]
    grads_out = [
        pltpu.make_async_copy(cstage.at[0], comp_k_grad.at[0, 0], gout_sem.at[0]),
        pltpu.make_async_copy(cstage.at[1], comp_v_grad.at[0, 0], gout_sem.at[1]),
    ]
    for c in grads_out:
        c.start()

    pltpu.make_async_copy(zrecv.at[1:nz], zrecv.at[1:nz], z_recv).wait()
    total = zf[0]
    for s in range(1, nz):
        total += zrecv[s].astype(F32)
    for k, ref in enumerate((prompt_k_grad, prompt_v_grad)):
        for g in range(groups):
            ref[0, :, g * HEAD_DIM : (g + 1) * HEAD_DIM] = total[k * groups + g : k * groups + g + 1, :]

    for c in list(first_leg.values()) + second_leg + column_legs:
        c.wait_send()
    for d in range(1, nx):

        @pl.when(x + d < nx)
        def _(d=d):
            kv_copy(d).wait_send()

        for g in range(groups):
            x_copy(g, d).wait_send()
    pltpu.make_async_copy(zsend.at[1:nz], zsend.at[1:nz], z_send).wait()

    @pl.loop(0, x)
    def _(b):
        for g in range(groups):
            remote(
                csend.at[b, g], crecv.at[0, g], c_send.at[b, g], c_recv.at[0, g], at_x(1)
            ).wait_send()

    pltpu.make_async_copy(o_half, o_half, out_sem.at[0]).wait()
    pltpu.make_async_copy(dq_half, dq_half, out_sem.at[1]).wait()
    for c in grads_out:
        c.wait()


def solution(mesh):
    nz, nx = mesh.shape["sample"], mesh.shape["fsdp"]

    def shards(queries, comp_k, comp_v, prompt_k, prompt_v, output_grad, lengths):
        count, width = queries.shape[2:]
        kv_width = comp_k.shape[3]
        groups = kv_width // HEAD_DIM
        heads = width // HEAD_DIM
        wide = heads // groups * count
        key_count = nz * nx
        reach = nz // 4
        blocks = nx + 1
        anywhere = pl.BlockSpec(memory_space=pl.ANY)
        vmem = pl.BlockSpec(memory_space=pltpu.VMEM)
        smem = pl.BlockSpec(memory_space=pltpu.SMEM)
        dma = pltpu.SemaphoreType.DMA
        one = jax.ShapeDtypeStruct
        return pl.pallas_call(
            functools.partial(kernel, nz, nx),
            out_shape=(
                one(queries.shape, BF16),
                one(queries.shape, BF16),
                one(comp_k.shape, F32),
                one(comp_k.shape, F32),
                one(prompt_k.shape, F32),
                one(prompt_k.shape, F32),
            ),
            in_specs=[anywhere, anywhere, anywhere, vmem, vmem, anywhere, smem],
            out_specs=(anywhere, anywhere, anywhere, anywhere, vmem, vmem),
            scratch_shapes=[
                pltpu.VMEM((heads * count, HEAD_DIM), BF16),
                pltpu.VMEM((heads * count, HEAD_DIM), BF16),
                pltpu.VMEM((blocks, 2, count, kv_width), BF16),
                pltpu.VMEM((blocks, 2, kv_width, count), BF16),
                pltpu.VMEM((nx, nz, 2 * groups, HEAD_DIM), BF16),
                pltpu.VMEM((key_count, 2 * groups, HEAD_DIM), F32),
                pltpu.VMEM((groups * blocks, count, wide), F32),
                pltpu.VMEM((groups * blocks, count, wide), F32),
                pltpu.VMEM((groups, HEAD_DIM, wide), F32),
                pltpu.VMEM((groups, HEAD_DIM, wide), F32),
                pltpu.VMEM((groups, 8, wide), F32),
                pltpu.VMEM((groups * blocks, 1, wide), F32),
                pltpu.VMEM((count, wide), BF16),
                pltpu.VMEM((count, wide), BF16),
                pltpu.VMEM((heads * count, HEAD_DIM), BF16),
                pltpu.VMEM((heads * count, HEAD_DIM), BF16),
                pltpu.VMEM((nx, groups, 2, count, HEAD_DIM), BF16),
                pltpu.VMEM((nx - 1, groups, 2, count, HEAD_DIM), BF16),
                pltpu.VMEM((groups, 2, count, HEAD_DIM), F32),
                pltpu.VMEM((2, count, kv_width), F32),
                pltpu.VMEM((groups, nx, 2, nz, HEAD_DIM), BF16),
                pltpu.VMEM((groups, 2, nz, HEAD_DIM), F32),
                pltpu.VMEM((groups, nx, 2, nz, HEAD_DIM), BF16),
                pltpu.VMEM((nz, 2 * groups, HEAD_DIM), F32),
                pltpu.VMEM((nz, 2 * groups, HEAD_DIM), BF16),
                pltpu.VMEM((nz, 2 * groups, HEAD_DIM), BF16),
                pltpu.VMEM((2 * groups, HEAD_DIM), F32),
                dma((2, groups)),
                dma((2,)),
                dma((2,)),
                dma((2,)),
                dma((2 * reach,)),
                dma((2 * reach,)),
                dma((2, reach)),
                dma((2, reach)),
                dma((3, nx - 1)),
                dma((3, nx - 1)),
                dma((nx - 1,)),
                dma((nx - 1,)),
                dma((groups, nx - 1)),
                dma((groups, nx - 1)),
                dma,
                dma,
                dma((nx, groups)),
                dma((nx - 1, groups)),
            ],
            compiler_params=pltpu.CompilerParams(
                collective_id=0, has_side_effects=True, vmem_limit_bytes=60 * 2**20
            ),
            name="attend",
        )(queries, comp_k, comp_v, prompt_k, prompt_v, output_grad, lengths)

    rows = P(("groups", "prompt"), "sample", "fsdp", None)
    prompt_rows = P(("groups", "prompt"), ("sample", "fsdp"), None)
    return jax.shard_map(
        shards,
        mesh=mesh,
        in_specs=(rows, rows, rows, prompt_rows, prompt_rows, rows, P(("groups", "prompt"), "sample")),
        out_specs=(rows, rows, rows, rows, prompt_rows, prompt_rows),
        check_vma=False,
    )
```

```python
import functools
import math

import jax
import jax.numpy as jnp
from jax import lax
from jax.experimental import pallas as pl
from jax.experimental.pallas import tpu as pltpu
from jax.sharding import PartitionSpec as P

HEAD_DIM = 128
TILE = 256
MESH = pl.DeviceIdType.MESH
F32 = jnp.float32
BF16 = jnp.bfloat16
NT = (((1,), (1,)), ((), ()))
NN = (((1,), (0,)), ((), ()))


def dot(a, b, dims=NN):
    return lax.dot_general(a, b, dims, preferred_element_type=F32)


def kernel(
    nz,
    nx,
    queries,
    comp_k,
    comp_v,
    prompt_k,
    prompt_v,
    out_grad,
    lengths,
    out,
    query_grad,
    comp_k_grad,
    comp_v_grad,
    prompt_k_grad,
    prompt_v_grad,
    q_s,
    g_s,
    kv,
    kvt,
    rows,
    rows32,
    e_s,
    dp_s,
    o_s,
    dq_s,
    stat,
    blockmax,
    p_half,
    ds_half,
    pp_s,
    dsp_s,
    csend,
    crecv,
    cown,
    xsend,
    xown,
    xrecv,
    zf,
    zsend,
    zrecv,
    pstage,
    in_sem,
    kvin_sem,
    r1_send,
    r1_recv,
    r2_send,
    r2_recv,
    rx_send,
    rx_recv,
    kv_send,
    kv_recv,
    x_send,
    x_recv,
    z_send,
    z_recv,
    c_send,
    c_recv,
):
    z = lax.axis_index("sample")
    x = lax.axis_index("fsdp")
    count = comp_k.shape[2]
    groups = comp_k.shape[3] // HEAD_DIM
    heads = queries.shape[3] // HEAD_DIM
    share = heads // groups
    wide = share * count
    reach = nz // 4
    scale = HEAD_DIM**-0.5
    fold = scale * math.log2(math.e)
    last = nx
    key_count = nz * nx

    def at_z(d):
        return {"sample": lax.rem(z + (d + nz) % nz, nz)}

    def at_x(d):
        return {"fsdp": lax.rem(x + d, nx)}

    def remote(src, dst, send, recv, to):
        return pltpu.make_async_remote_copy(
            src_ref=src, dst_ref=dst, send_sem=send, recv_sem=recv, device_id=to, device_id_type=MESH
        )

    own_kv = [
        pltpu.make_async_copy(comp_k.at[0, 0], kv.at[x, 0], kvin_sem.at[0]),
        pltpu.make_async_copy(comp_v.at[0, 0], kv.at[x, 1], kvin_sem.at[1]),
    ]
    for c in own_kv:
        c.start()

    @pl.loop(0, groups)
    def _(g):
        for h in range(share):
            head = g * share + h
            cols = pl.ds(pl.multiple_of(head * HEAD_DIM, HEAD_DIM), HEAD_DIM)
            dst = pl.ds(pl.multiple_of(head * count, count), count)
            pltpu.make_async_copy(queries.at[0, 0, :, cols], q_s.at[dst], in_sem.at[0, g]).start()
            pltpu.make_async_copy(out_grad.at[0, 0, :, cols], g_s.at[dst], in_sem.at[1, g]).start()

    for k, ref in enumerate((prompt_k, prompt_v)):
        row = ref[0].astype(F32)
        for g in range(groups):
            pstage[k * groups + g : k * groups + g + 1, :] = row[:, g * HEAD_DIM : (g + 1) * HEAD_DIM]
    rows[0, 0] = pstage[...].astype(BF16)

    barrier = pltpu.get_barrier_semaphore()
    near = [d for d in range(1, reach + 1)] + [-d for d in range(1, reach + 1)]
    for d in near:
        pl.semaphore_signal(barrier, inc=1, device_id=at_z(d), device_id_type=MESH)
    for d in range(1, nx):
        pl.semaphore_signal(barrier, inc=1, device_id=at_x(d), device_id_type=MESH)

    def turn(b):
        for part in range(2):
            for g in range(groups):
                cols = slice(g * HEAD_DIM, (g + 1) * HEAD_DIM)
                kvt[b, part, cols, :] = kv[b, part, :, cols].astype(F32).T.astype(BF16)

    def forward(b, g, first):
        cols = pl.ds(pl.multiple_of(g * HEAD_DIM, HEAD_DIM), HEAD_DIM)
        keys = kv[b, 0, :, cols]
        values = kv[b, 1, :, cols]
        values_t = kvt[b, 1, cols, :]
        slot = g * nx + b
        for t in range(wide // TILE):
            at = slice(t * TILE, (t + 1) * TILE)
            src = pl.ds(pl.multiple_of(g * wide + t * TILE, TILE), TILE)
            s = dot(keys, q_s[src, :], NT)
            if first:
                key = lax.broadcasted_iota(jnp.int32, s.shape, 0)
                token = lax.broadcasted_iota(jnp.int32, s.shape, 1) % count
                s = jnp.where(key <= token, s, -1e30)
            top = jnp.max(s, axis=0, keepdims=True)
            if not first:
                before = stat[g, 0:1, at]
                top = jnp.maximum(top, before)
            e = jnp.exp2((s - top) * fold)
            total = jnp.sum(e, axis=0, keepdims=True)
            dp = dot(values, g_s[src, :], NT)
            mean = jnp.sum(e * dp, axis=0, keepdims=True)
            o = dot(values_t, e.astype(BF16))
            if not first:
                old = jnp.exp2((before - top) * fold)
                total += old * stat[g, 1:2, at]
                mean += old * stat[g, 2:3, at]
                o += old * o_s[g, :, at]
            stat[g, 0:1, at] = top
            stat[g, 1:2, at] = total
            stat[g, 2:3, at] = mean
            o_s[g, :, at] = o
            e_s[slot, :, at] = e
            dp_s[slot, :, at] = dp
            blockmax[slot, 0:1, at] = top

    def backward(b, g, first):
        cols = pl.ds(pl.multiple_of(g * HEAD_DIM, HEAD_DIM), HEAD_DIM)
        keys_t = kvt[b, 0, cols, :]
        slot = g * nx + b
        for t in range(wide // TILE):
            at = slice(t * TILE, (t + 1) * TILE)
            factor = jnp.exp2((blockmax[slot, 0:1, at] - stat[g, 0:1, at]) * fold) * stat[g, 1:2, at]
            p = e_s[slot, :, at] * factor
            ds = (p * (dp_s[slot, :, at] - stat[g, 2:3, at])).astype(BF16)
            p_half[:, at] = p.astype(BF16)
            ds_half[:, at] = ds
            dq = dot(keys_t, ds)
            if first:
                dq += dot(kvt[last, 0, cols, :], dsp_s[g, :, at])
                dq_s[g, :, at] = dq
            else:
                dq_s[g, :, at] += dq
        src = pl.ds(pl.multiple_of(g * wide, wide), wide)
        return dot(ds_half[...], q_s[src, :]) * scale, dot(p_half[...], g_s[src, :])

    def flush(source, target, g):
        for t in range(wide // TILE):
            block = source(slice(t * TILE, (t + 1) * TILE)).T.astype(BF16)
            for h in range(TILE // count):
                head = g * share + t * (TILE // count) + h
                cols = pl.ds(pl.multiple_of(head * HEAD_DIM, HEAD_DIM), HEAD_DIM)
                target[0, 0, :, cols] = block[h * count : (h + 1) * count]

    pl.semaphore_wait(barrier, len(near) + nx - 1)

    first_leg = {
        d: remote(
            rows.at[0, 0], rows.at[0, (nz - d) % nz], r1_send.at[n], r1_recv.at[n], at_z(d)
        )
        for n, d in enumerate(near)
    }
    for d in sorted(near, key=abs, reverse=True):
        first_leg[d].start()

    def kv_copy(d):
        return remote(kv.at[x], kv.at[x], kv_send.at[d - 1], kv_recv.at[d - 1], at_x(d))

    for c in own_kv:
        c.wait()
    for d in range(1, nx):

        @pl.when(x + d < nx)
        def _(d=d):
            kv_copy(d).start()

    turn(x)
    token = lax.broadcasted_iota(jnp.int32, (count, HEAD_DIM), 0) + x * count
    length = jnp.full((count, HEAD_DIM), lengths[0, 0], jnp.int32)
    weight = jnp.where(token < length, F32(count * nx) / length.astype(F32), 0.0)

    @pl.loop(0, groups)
    def _(g):
        src = pl.ds(pl.multiple_of(g * wide, wide), wide)
        pltpu.make_async_copy(q_s.at[src], q_s.at[src], in_sem.at[0, g]).wait()
        pltpu.make_async_copy(g_s.at[src], g_s.at[src], in_sem.at[1, g]).wait()
        for h in range(share):
            at = pl.ds(pl.multiple_of((g * share + h) * count, count), count)
            g_s[at, :] = (g_s[at, :].astype(F32) * weight).astype(BF16)
        forward(x, g, True)

    second_leg = []
    for e in range(1, reach + 1):
        first_leg[-e].wait_recv()
        c = remote(
            rows.at[0, e], rows.at[0, reach + e], r2_send.at[0, e - 1], r2_recv.at[0, e - 1], at_z(-reach)
        )
        c.start()
        second_leg.append(c)
        first_leg[e].wait_recv()
        if e < reach:
            c = remote(
                rows.at[0, nz - e],
                rows.at[0, nz - reach - e],
                r2_send.at[1, e - 1],
                r2_recv.at[1, e - 1],
                at_z(reach),
            )
            c.start()
            second_leg.append(c)

    def to_columns(part, begin, end):
        return [
            remote(
                rows.at[0, begin:end],
                rows.at[nx - d, begin:end],
                rx_send.at[part, d - 1],
                rx_recv.at[part, d - 1],
                at_x(d),
            )
            for d in range(1, nx)
        ]

    column_legs = to_columns(0, 0, reach + 1) + to_columns(1, nz - reach, nz)
    for c in column_legs:
        c.start()

    @pl.loop(0, x)
    def _(n):
        d = n + 1
        b = x - d
        remote(kv.at[b], kv.at[b], kv_send.at[n], kv_recv.at[n], at_x(1)).wait_recv()
        turn(b)

        @pl.loop(0, groups)
        def _(g):
            forward(b, g, False)

    ahead, behind = second_leg[0::2], second_leg[1::2]
    ahead += behind[reach - 1 :]
    behind = behind[: reach - 1]
    half = reach // 2
    pieces = [
        (ahead[:half], reach + 1, reach + 1 + half),
        (behind[:half], nz - reach - half, nz - reach),
        (ahead[half:], reach + 1 + half, 2 * reach + 1),
        (behind[half:], 2 * reach + 1, nz - reach - half),
    ]
    for n, (arrivals, begin, end) in enumerate(pieces):
        for c in arrivals:
            c.wait_recv()
        if end > begin:
            legs = to_columns(2 + n, begin, end)
            for c in legs:
                c.start()
            column_legs += legs
    for c in column_legs:
        c.wait_recv()

    for d in range(nx):
        part_rows = nz * 2 * groups
        rows32[d * part_rows : (d + 1) * part_rows, :] = rows[d].astype(F32).reshape(part_rows, HEAD_DIM)
    for part in range(2):
        for g in range(groups):
            cols = slice(g * HEAD_DIM, (g + 1) * HEAD_DIM)
            block = rows32[pl.ds(part * groups + g, key_count, stride=2 * groups), :]
            kv[last, part, :, cols] = block.astype(BF16)
            kvt[last, part, cols, :] = block.T.astype(BF16)

    def x_copy(g, d):
        return remote(
            xsend.at[g, d], xrecv.at[g, nx - d], x_send.at[g, d - 1], x_recv.at[g, d - 1], at_x(d)
        )

    @pl.loop(0, groups)
    def _(g):
        cols = pl.ds(pl.multiple_of(g * HEAD_DIM, HEAD_DIM), HEAD_DIM)
        keys = kv[last, 0, :, cols]
        values = kv[last, 1, :, cols]
        for t in range(wide // TILE):
            at = slice(t * TILE, (t + 1) * TILE)
            src = pl.ds(pl.multiple_of(g * wide + t * TILE, TILE), TILE)
            s = dot(keys, q_s[src, :], NT)
            before = stat[g, 0:1, at]
            top = jnp.maximum(jnp.max(s, axis=0, keepdims=True), before)
            e = jnp.exp2((s - top) * fold)
            old = jnp.exp2((before - top) * fold)
            inverse = 1.0 / (old * stat[g, 1:2, at] + jnp.sum(e, axis=0, keepdims=True))
            dp = dot(values, g_s[src, :], NT)
            p = e * inverse
            mean = old * inverse * stat[g, 2:3, at] + jnp.sum(p * dp, axis=0, keepdims=True)
            pp_s[g, :, at] = p.astype(BF16)
            dsp_s[g, :, at] = (p * (dp - mean)).astype(BF16)
            stat[g, 0:1, at] = top
            stat[g, 1:2, at] = inverse
            stat[g, 2:3, at] = mean
            stat[g, 3:4, at] = old * inverse
        src = pl.ds(pl.multiple_of(g * wide, wide), wide)
        both = dot(dsp_s[g], q_s[src, :]) * scale, dot(pp_s[g], g_s[src, :])
        for part in range(2):
            xown[g, part] = both[part][:nz]
            for d in range(1, nx):
                xsend[g, d, part] = both[part][d * nz : (d + 1) * nz].astype(BF16)
        for d in range(1, nx):
            x_copy(g, d).start()

    def c_copy(b, g, d):
        return remote(
            csend.at[b, g], crecv.at[d - 1, g], c_send.at[b, g], c_recv.at[d - 1, g], {"fsdp": b}
        )

    def completion_backward(b, first):
        @pl.loop(0, groups)
        def _(g):
            both = backward(b, g, first)

            @pl.when(b < x)
            def _():
                for part in range(2):
                    csend[b, g, part] = both[part].astype(BF16)
                c_copy(b, g, x - b).start()

            @pl.when(b == x)
            def _():
                for part in range(2):
                    cown[g, part] = both[part]

    completion_backward(0, True)

    for g in range(groups):
        for d in range(1, nx):
            x_copy(g, d).wait_recv()
    for g in range(groups):
        for part in range(2):
            total = xown[g, part]
            for d in range(1, nx):
                total += xrecv[g, d, part].astype(F32)
            zf[pl.ds(part * groups + g, nz, stride=2 * groups), :] = total
    zsend[...] = zf[...].reshape(nz, 2 * groups, HEAD_DIM).astype(BF16)

    def z_copy(s):
        return remote(zsend.at[s], zrecv.at[nz - s], z_send, z_recv, at_z(s))

    for s in sorted(range(1, nz), key=lambda s: min(s, nz - s), reverse=True):
        z_copy(s).start()

    @pl.loop(1, x + 1)
    def _(b):
        completion_backward(b, False)

    @pl.loop(0, groups)
    def _(g):
        cols = pl.ds(pl.multiple_of(g * HEAD_DIM, HEAD_DIM), HEAD_DIM)
        values_t = kvt[last, 1, cols, :]
        flush(
            lambda at: o_s[g, :, at] * stat[g, 3:4, at] + dot(values_t, pp_s[g, :, at]),
            out,
            g,
        )

    @pl.loop(0, groups)
    def _(g):
        flush(lambda at: dq_s[g, :, at] * scale, query_grad, g)

    for d in range(1, nx):

        @pl.when(x + d < nx)
        def _(d=d):
            for g in range(groups):
                remote(
                    csend.at[0, g], crecv.at[d - 1, g], c_send.at[0, g], c_recv.at[d - 1, g], at_x(d)
                ).wait_recv()
                for part in range(2):
                    cown[g, part] += crecv[d - 1, g, part].astype(F32)

    for part, ref in enumerate((comp_k_grad, comp_v_grad)):
        for g in range(groups):
            ref[0, 0, :, g * HEAD_DIM : (g + 1) * HEAD_DIM] = cown[g, part]

    for c in list(first_leg.values()) + second_leg + column_legs:
        c.wait_send()
    for d in range(1, nx):

        @pl.when(x + d < nx)
        def _(d=d):
            kv_copy(d).wait_send()

        for g in range(groups):
            x_copy(g, d).wait_send()
    pltpu.make_async_copy(zsend.at[1:nz], zsend.at[1:nz], z_send).wait()

    @pl.loop(0, x)
    def _(b):
        for g in range(groups):
            remote(
                csend.at[b, g], crecv.at[0, g], c_send.at[b, g], c_recv.at[0, g], at_x(1)
            ).wait_send()

    pltpu.make_async_copy(zrecv.at[1:nz], zrecv.at[1:nz], z_recv).wait()
    total = zf[: 2 * groups, :]
    for s in range(1, nz):
        total += zrecv[s].astype(F32)
    for k, ref in enumerate((prompt_k_grad, prompt_v_grad)):
        for g in range(groups):
            ref[0, :, g * HEAD_DIM : (g + 1) * HEAD_DIM] = total[k * groups + g : k * groups + g + 1, :]


def hand_on(*refs):
    n = len(refs) // 2
    sem = refs[-1]
    copies = [pltpu.make_async_copy(refs[k], refs[n + k], sem.at[k]) for k in range(n)]
    for c in copies:
        c.start()
    for c in copies:
        c.wait()


def solution(mesh):
    nz, nx = mesh.shape["sample"], mesh.shape["fsdp"]

    def shards(queries, comp_k, comp_v, prompt_k, prompt_v, output_grad, lengths):
        count, width = queries.shape[2:]
        kv_width = comp_k.shape[3]
        groups = kv_width // HEAD_DIM
        heads = width // HEAD_DIM
        wide = heads // groups * count
        key_count = nz * nx
        reach = nz // 4
        blocks = nx + 1
        anywhere = pl.BlockSpec(memory_space=pl.ANY)
        vmem = pl.BlockSpec(memory_space=pltpu.VMEM)
        smem = pl.BlockSpec(memory_space=pltpu.SMEM)
        dma = pltpu.SemaphoreType.DMA
        one = jax.ShapeDtypeStruct
        results = pl.pallas_call(
            functools.partial(kernel, nz, nx),
            out_shape=(
                pltpu.VMEM(queries.shape, BF16),
                pltpu.VMEM(queries.shape, BF16),
                pltpu.VMEM(comp_k.shape, F32),
                pltpu.VMEM(comp_k.shape, F32),
                pltpu.VMEM(prompt_k.shape, F32),
                pltpu.VMEM(prompt_k.shape, F32),
            ),
            in_specs=[anywhere, anywhere, anywhere, vmem, vmem, anywhere, smem],
            out_specs=(vmem,) * 6,
            scratch_shapes=[
                pltpu.VMEM((heads * count, HEAD_DIM), BF16),
                pltpu.VMEM((heads * count, HEAD_DIM), BF16),
                pltpu.VMEM((blocks, 2, count, kv_width), BF16),
                pltpu.VMEM((blocks, 2, kv_width, count), BF16),
                pltpu.VMEM((nx, nz, 2 * groups, HEAD_DIM), BF16),
                pltpu.VMEM((key_count * 2 * groups, HEAD_DIM), F32),
                pltpu.VMEM((groups * nx, count, wide), F32),
                pltpu.VMEM((groups * nx, count, wide), F32),
                pltpu.VMEM((groups, HEAD_DIM, wide), F32),
                pltpu.VMEM((groups, HEAD_DIM, wide), F32),
                pltpu.VMEM((groups, 8, wide), F32),
                pltpu.VMEM((groups * nx, 1, wide), F32),
                pltpu.VMEM((count, wide), BF16),
                pltpu.VMEM((count, wide), BF16),
                pltpu.VMEM((groups, key_count, wide), BF16),
                pltpu.VMEM((groups, key_count, wide), BF16),
                pltpu.VMEM((nx, groups, 2, count, HEAD_DIM), BF16),
                pltpu.VMEM((nx - 1, groups, 2, count, HEAD_DIM), BF16),
                pltpu.VMEM((groups, 2, count, HEAD_DIM), F32),
                pltpu.VMEM((groups, nx, 2, nz, HEAD_DIM), BF16),
                pltpu.VMEM((groups, 2, nz, HEAD_DIM), F32),
                pltpu.VMEM((groups, nx, 2, nz, HEAD_DIM), BF16),
                pltpu.VMEM((nz * 2 * groups, HEAD_DIM), F32),
                pltpu.VMEM((nz, 2 * groups, HEAD_DIM), BF16),
                pltpu.VMEM((nz, 2 * groups, HEAD_DIM), BF16),
                pltpu.VMEM((2 * groups, HEAD_DIM), F32),
                dma((2, groups)),
                dma((2,)),
                dma((2 * reach,)),
                dma((2 * reach,)),
                dma((2, reach)),
                dma((2, reach)),
                dma((6, nx - 1)),
                dma((6, nx - 1)),
                dma((nx - 1,)),
                dma((nx - 1,)),
                dma((groups, nx - 1)),
                dma((groups, nx - 1)),
                dma,
                dma,
                dma((nx, groups)),
                dma((nx - 1, groups)),
            ],
            compiler_params=pltpu.CompilerParams(
                collective_id=0, has_side_effects=True, vmem_limit_bytes=58 * 2**20
            ),
            name="attend",
        )(queries, comp_k, comp_v, prompt_k, prompt_v, output_grad, lengths)
        n = len(results)
        return pl.pallas_call(
            hand_on,
            out_shape=tuple(one(r.shape, r.dtype) for r in results),
            in_specs=[vmem] * n,
            out_specs=(anywhere,) * n,
            scratch_shapes=[dma((n,))],
            compiler_params=pltpu.CompilerParams(vmem_limit_bytes=2**20),
            name="hand_on",
        )(*(pltpu.with_memory_space_constraint(r, pltpu.VMEM) for r in results))

    rows = P(("groups", "prompt"), "sample", "fsdp", None)
    prompt_rows = P(("groups", "prompt"), ("sample", "fsdp"), None)
    return jax.shard_map(
        shards,
        mesh=mesh,
        in_specs=(rows, rows, rows, prompt_rows, prompt_rows, rows, P(("groups", "prompt"), "sample")),
        out_specs=(rows, rows, rows, rows, prompt_rows, prompt_rows),
        check_vma=False,
    )
```

```python
import functools
import math

import jax
import jax.numpy as jnp
from jax import lax
from jax.experimental import pallas as pl
from jax.experimental.pallas import tpu as pltpu
from jax.sharding import PartitionSpec as P

HEAD_DIM = 128
TILE = 256
MESH = pl.DeviceIdType.MESH
F32 = jnp.float32
BF16 = jnp.bfloat16


def dot(a, b):
    return jnp.dot(a, b, preferred_element_type=F32)


def kernel(
    nz,
    nx,
    queries,
    comp_k,
    comp_v,
    prompt_k,
    prompt_v,
    out_grad,
    lengths,
    out,
    query_grad,
    comp_k_grad,
    comp_v_grad,
    prompt_k_grad,
    prompt_v_grad,
    q_s,
    g_s,
    qt_s,
    gt_s,
    kv,
    kvt,
    rows,
    rows32,
    e_s,
    dp_s,
    o_s,
    dq_s,
    stat,
    blockmax,
    p_half,
    ds_half,
    pp_s,
    dsp_s,
    csend,
    crecv,
    cown,
    xsend,
    xown,
    xrecv,
    zf,
    zsend,
    zrecv,
    pstage,
    pin,
    in_sem,
    kvin_sem,
    pin_sem,
    r1_send,
    r1_recv,
    r2_send,
    r2_recv,
    rx_send,
    rx_recv,
    kv_send,
    kv_recv,
    x_send,
    x_recv,
    z_send,
    z_recv,
    c_send,
    c_recv,
):
    z = lax.axis_index("sample")
    x = lax.axis_index("fsdp")
    count = comp_k.shape[2]
    groups = comp_k.shape[3] // HEAD_DIM
    heads = queries.shape[3] // HEAD_DIM
    share = heads // groups
    wide = share * count
    tiles = wide // TILE
    reach = nz // 4
    scale = HEAD_DIM**-0.5
    fold = scale * math.log2(math.e)
    last = nx
    key_count = nz * nx

    def at_z(d):
        return {"sample": lax.rem(z + (d + nz) % nz, nz)}

    def at_x(d):
        return {"fsdp": lax.rem(x + d, nx)}

    def remote(src, dst, send, recv, to):
        return pltpu.make_async_remote_copy(
            src_ref=src, dst_ref=dst, send_sem=send, recv_sem=recv, device_id=to, device_id_type=MESH
        )

    barrier = pltpu.get_barrier_semaphore()
    near = [d for d in range(1, reach + 1)] + [-d for d in range(1, reach + 1)]
    for d in near:
        pl.semaphore_signal(barrier, inc=1, device_id=at_z(d), device_id_type=MESH)
    for d in range(1, nx):
        pl.semaphore_signal(barrier, inc=1, device_id=at_x(d), device_id_type=MESH)

    own_kv = [
        pltpu.make_async_copy(comp_k.at[0, 0], kv.at[x, 0], kvin_sem.at[0]),
        pltpu.make_async_copy(comp_v.at[0, 0], kv.at[x, 1], kvin_sem.at[1]),
    ]
    own_rows = [
        pltpu.make_async_copy(prompt_k, pin.at[0], pin_sem.at[0]),
        pltpu.make_async_copy(prompt_v, pin.at[1], pin_sem.at[1]),
    ]
    for c in own_rows + own_kv:
        c.start()

    @pl.loop(0, groups)
    def _(g):
        for h in range(share):
            head = g * share + h
            cols = pl.ds(pl.multiple_of(head * HEAD_DIM, HEAD_DIM), HEAD_DIM)
            dst = pl.ds(pl.multiple_of(head * count, count), count)
            pltpu.make_async_copy(queries.at[0, 0, :, cols], q_s.at[dst], in_sem.at[0, g]).start()
            pltpu.make_async_copy(out_grad.at[0, 0, :, cols], g_s.at[dst], in_sem.at[1, g]).start()

    for k in range(2):
        own_rows[k].wait()
        row = pin[k, 0].astype(F32)
        for g in range(groups):
            pstage[k * groups + g : k * groups + g + 1, :] = row[:, g * HEAD_DIM : (g + 1) * HEAD_DIM]
    rows[0, 0] = pstage[...].astype(BF16)

    def turn(b, begin, end):
        for part in range(2):
            for g in range(begin, end):
                cols = slice(g * HEAD_DIM, (g + 1) * HEAD_DIM)
                kvt[b, part, cols, :] = kv[b, part, :, cols].astype(F32).T.astype(BF16)

    def forward(b, g, first):
        cols = pl.ds(pl.multiple_of(g * HEAD_DIM, HEAD_DIM), HEAD_DIM)
        keys = kv[b, 0, :, cols]
        values = kv[b, 1, :, cols]
        values_t = kvt[b, 1, cols, :]
        slot = g * nx + b
        for t in range(tiles):
            at = slice(t * TILE, (t + 1) * TILE)
            s = dot(keys, qt_s[g * tiles + t])
            if first:
                key = lax.broadcasted_iota(jnp.int32, s.shape, 0)
                token = lax.broadcasted_iota(jnp.int32, s.shape, 1) % count
                s = jnp.where(key <= token, s, -1e30)
            top = jnp.max(s, axis=0, keepdims=True)
            if not first:
                before = stat[g, 0:1, at]
                top = jnp.maximum(top, before)
            e = jnp.exp2((s - top) * fold)
            total = jnp.sum(e, axis=0, keepdims=True)
            dp = dot(values, gt_s[g * tiles + t])
            mean = jnp.sum(e * dp, axis=0, keepdims=True)
            o = dot(values_t, e.astype(BF16))
            if not first:
                old = jnp.exp2((before - top) * fold)
                total += old * stat[g, 1:2, at]
                mean += old * stat[g, 2:3, at]
                o += old * o_s[g, :, at]
            stat[g, 0:1, at] = top
            stat[g, 1:2, at] = total
            stat[g, 2:3, at] = mean
            o_s[g, :, at] = o
            e_s[slot, :, at] = e
            dp_s[slot, :, at] = dp
            blockmax[slot, 0:1, at] = top

    def backward(b, g, first):
        cols = pl.ds(pl.multiple_of(g * HEAD_DIM, HEAD_DIM), HEAD_DIM)
        keys_t = kvt[b, 0, cols, :]
        slot = g * nx + b
        for t in range(tiles):
            at = slice(t * TILE, (t + 1) * TILE)
            factor = jnp.exp2((blockmax[slot, 0:1, at] - stat[g, 0:1, at]) * fold) * stat[g, 1:2, at]
            p = e_s[slot, :, at] * factor
            ds = (p * (dp_s[slot, :, at] - stat[g, 2:3, at])).astype(BF16)
            p_half[:, at] = p.astype(BF16)
            ds_half[:, at] = ds
            dq = dot(keys_t, ds)
            if first:
                dq += dot(kvt[last, 0, cols, :], dsp_s[g, :, at])
                dq_s[g, :, at] = dq
            else:
                dq_s[g, :, at] += dq
        src = pl.ds(pl.multiple_of(g * wide, wide), wide)
        return dot(ds_half[...], q_s[src, :]) * scale, dot(p_half[...], g_s[src, :])

    def flush(source, target, g):
        for t in range(tiles):
            block = source(slice(t * TILE, (t + 1) * TILE)).T.astype(BF16)
            for h in range(TILE // count):
                head = g * share + t * (TILE // count) + h
                cols = pl.ds(pl.multiple_of(head * HEAD_DIM, HEAD_DIM), HEAD_DIM)
                target[0, 0, :, cols] = block[h * count : (h + 1) * count]

    pl.semaphore_wait(barrier, len(near) + nx - 1)

    first_leg = {
        d: remote(
            rows.at[0, 0], rows.at[0, (nz - d) % nz], r1_send.at[n], r1_recv.at[n], at_z(d)
        )
        for n, d in enumerate(near)
    }
    for d in sorted(near, key=abs, reverse=True):
        first_leg[d].start()

    middle = groups // 2

    def kv_copy(half, d, b):
        cols = pl.ds(half * middle * HEAD_DIM, middle * HEAD_DIM)
        block = kv.at[b, :, :, cols]
        return remote(block, block, kv_send.at[half, d - 1], kv_recv.at[half, d - 1], at_x(d))

    for c in own_kv:
        c.wait()
    for half in range(2):
        for d in range(1, nx):

            @pl.when(x + d < nx)
            def _(half=half, d=d):
                kv_copy(half, d, x).start()

    turn(x, 0, groups)
    token = lax.broadcasted_iota(jnp.int32, (count, HEAD_DIM), 0) + x * count
    length = jnp.full((count, HEAD_DIM), lengths[0, 0], jnp.int32)
    weight = jnp.where(token < length, F32(count * nx) / length.astype(F32), 0.0)

    @pl.loop(0, groups)
    def _(g):
        src = pl.ds(pl.multiple_of(g * wide, wide), wide)
        pltpu.make_async_copy(q_s.at[src], q_s.at[src], in_sem.at[0, g]).wait()
        pltpu.make_async_copy(g_s.at[src], g_s.at[src], in_sem.at[1, g]).wait()
        for h in range(share):
            at = pl.ds(pl.multiple_of((g * share + h) * count, count), count)
            g_s[at, :] = (g_s[at, :].astype(F32) * weight).astype(BF16)
        for t in range(tiles):
            src = pl.ds(pl.multiple_of(g * wide + t * TILE, TILE), TILE)
            qt_s[g * tiles + t] = q_s[src, :].astype(F32).T.astype(BF16)
            gt_s[g * tiles + t] = g_s[src, :].astype(F32).T.astype(BF16)
        forward(x, g, True)

    second_leg = []
    for e in range(1, reach + 1):
        first_leg[-e].wait_recv()
        c = remote(
            rows.at[0, e], rows.at[0, reach + e], r2_send.at[0, e - 1], r2_recv.at[0, e - 1], at_z(-reach)
        )
        c.start()
        second_leg.append(c)
        first_leg[e].wait_recv()
        if e < reach:
            c = remote(
                rows.at[0, nz - e],
                rows.at[0, nz - reach - e],
                r2_send.at[1, e - 1],
                r2_recv.at[1, e - 1],
                at_z(reach),
            )
            c.start()
            second_leg.append(c)

    def to_columns(part, begin, end):
        return [
            remote(
                rows.at[0, begin:end],
                rows.at[nx - d, begin:end],
                rx_send.at[part, d - 1],
                rx_recv.at[part, d - 1],
                at_x(d),
            )
            for d in range(1, nx)
        ]

    column_legs = to_columns(0, 0, reach + 1) + to_columns(1, nz - reach, nz)
    for c in column_legs:
        c.start()

    def earlier(half):
        @pl.loop(0, nx - 1)
        def _(n):
            d = lax.rem(n + nx - 2, nx - 1) + 1

            @pl.when(d <= x)
            def _():
                b = x - d
                cols = pl.ds(half * middle * HEAD_DIM, middle * HEAD_DIM)
                block = kv.at[b, :, :, cols]
                remote(
                    block, block, kv_send.at[half, d - 1], kv_recv.at[half, d - 1], at_x(1)
                ).wait_recv()
                turn(b, half * middle, (half + 1) * middle)

                @pl.loop(half * middle, (half + 1) * middle)
                def _(g):
                    forward(b, g, False)

    earlier(0)

    ahead, behind = second_leg[0::2], second_leg[1::2]
    ahead += behind[reach - 1 :]
    behind = behind[: reach - 1]
    half = reach // 2
    pieces = [
        (ahead[:half], reach + 1, reach + 1 + half),
        (behind[:half], nz - reach - half, nz - reach),
        (ahead[half:], reach + 1 + half, 2 * reach + 1),
        (behind[half:], 2 * reach + 1, nz - reach - half),
    ]
    for n, (arrivals, begin, end) in enumerate(pieces):
        for c in arrivals:
            c.wait_recv()
        if end > begin:
            legs = to_columns(2 + n, begin, end)
            for c in legs:
                c.start()
            column_legs += legs

    earlier(1)

    for c in column_legs:
        c.wait_recv()

    for d in range(nx):
        part_rows = nz * 2 * groups
        rows32[d * part_rows : (d + 1) * part_rows, :] = rows[d].astype(F32).reshape(part_rows, HEAD_DIM)
    for part in range(2):
        for g in range(groups):
            cols = slice(g * HEAD_DIM, (g + 1) * HEAD_DIM)
            block = rows32[pl.ds(part * groups + g, key_count, stride=2 * groups), :]
            kv[last, part, :, cols] = block.astype(BF16)
            kvt[last, part, cols, :] = block.T.astype(BF16)

    def x_copy(g, d):
        return remote(
            xsend.at[g, d], xrecv.at[g, nx - d], x_send.at[g, d - 1], x_recv.at[g, d - 1], at_x(d)
        )

    @pl.loop(0, groups)
    def _(g):
        cols = pl.ds(pl.multiple_of(g * HEAD_DIM, HEAD_DIM), HEAD_DIM)
        keys = kv[last, 0, :, cols]
        values = kv[last, 1, :, cols]
        for t in range(tiles):
            at = slice(t * TILE, (t + 1) * TILE)
            s = dot(keys, qt_s[g * tiles + t])
            before = stat[g, 0:1, at]
            top = jnp.maximum(jnp.max(s, axis=0, keepdims=True), before)
            e = jnp.exp2((s - top) * fold)
            old = jnp.exp2((before - top) * fold)
            inverse = 1.0 / (old * stat[g, 1:2, at] + jnp.sum(e, axis=0, keepdims=True))
            dp = dot(values, gt_s[g * tiles + t])
            p = e * inverse
            mean = old * inverse * stat[g, 2:3, at] + jnp.sum(p * dp, axis=0, keepdims=True)
            pp_s[g, :, at] = p.astype(BF16)
            dsp_s[g, :, at] = (p * (dp - mean)).astype(BF16)
            stat[g, 0:1, at] = top
            stat[g, 1:2, at] = inverse
            stat[g, 2:3, at] = mean
            stat[g, 3:4, at] = old * inverse
        src = pl.ds(pl.multiple_of(g * wide, wide), wide)
        both = dot(dsp_s[g], q_s[src, :]) * scale, dot(pp_s[g], g_s[src, :])
        for part in range(2):
            xown[g, part] = both[part][:nz]
            for d in range(1, nx):
                xsend[g, d, part] = both[part][d * nz : (d + 1) * nz].astype(BF16)
        for d in range(1, nx):
            x_copy(g, d).start()

    def c_copy(b, g, d):
        return remote(
            csend.at[b, g], crecv.at[d - 1, g], c_send.at[b, g], c_recv.at[d - 1, g], {"fsdp": b}
        )

    def completion_backward(b, first):
        @pl.loop(0, groups)
        def _(g):
            both = backward(b, g, first)

            @pl.when(b < x)
            def _():
                for part in range(2):
                    csend[b, g, part] = both[part].astype(BF16)
                c_copy(b, g, x - b).start()

            @pl.when(b == x)
            def _():
                for part in range(2):
                    cown[g, part] = both[part]

    completion_backward(x, True)

    for g in range(groups):
        for d in range(1, nx):
            x_copy(g, d).wait_recv()
    for g in range(groups):
        for part in range(2):
            total = xown[g, part]
            for d in range(1, nx):
                total += xrecv[g, d, part].astype(F32)
            zf[pl.ds(part * groups + g, nz, stride=2 * groups), :] = total
    zsend[...] = zf[...].reshape(nz, 2 * groups, HEAD_DIM).astype(BF16)

    def z_copy(s):
        return remote(zsend.at[s], zrecv.at[nz - s], z_send, z_recv, at_z(s))

    for s in sorted(range(1, nz), key=lambda s: min(s, nz - s), reverse=True):
        z_copy(s).start()

    @pl.loop(0, x)
    def _(b):
        completion_backward(b, False)

    @pl.loop(0, groups)
    def _(g):
        cols = pl.ds(pl.multiple_of(g * HEAD_DIM, HEAD_DIM), HEAD_DIM)
        values_t = kvt[last, 1, cols, :]
        flush(
            lambda at: o_s[g, :, at] * stat[g, 3:4, at] + dot(values_t, pp_s[g, :, at]),
            out,
            g,
        )

    @pl.loop(0, groups)
    def _(g):
        flush(lambda at: dq_s[g, :, at] * scale, query_grad, g)

    for d in range(1, nx):

        @pl.when(x + d < nx)
        def _(d=d):
            for g in range(groups):
                remote(
                    csend.at[0, g], crecv.at[d - 1, g], c_send.at[0, g], c_recv.at[d - 1, g], at_x(d)
                ).wait_recv()
                for part in range(2):
                    cown[g, part] += crecv[d - 1, g, part].astype(F32)

    for part, ref in enumerate((comp_k_grad, comp_v_grad)):
        for g in range(groups):
            ref[0, 0, :, g * HEAD_DIM : (g + 1) * HEAD_DIM] = cown[g, part]

    for c in list(first_leg.values()) + second_leg + column_legs:
        c.wait_send()
    for d in range(1, nx):

        @pl.when(x + d < nx)
        def _(d=d):
            for half in range(2):
                kv_copy(half, d, x).wait_send()

        for g in range(groups):
            x_copy(g, d).wait_send()
    pltpu.make_async_copy(zsend.at[1:nz], zsend.at[1:nz], z_send).wait()

    @pl.loop(0, x)
    def _(b):
        for g in range(groups):
            remote(
                csend.at[b, g], crecv.at[0, g], c_send.at[b, g], c_recv.at[0, g], at_x(1)
            ).wait_send()

    pltpu.make_async_copy(zrecv.at[1:nz], zrecv.at[1:nz], z_recv).wait()
    total = zf[: 2 * groups, :]
    for s in range(1, nz):
        total += zrecv[s].astype(F32)
    for k, ref in enumerate((prompt_k_grad, prompt_v_grad)):
        for g in range(groups):
            ref[0, :, g * HEAD_DIM : (g + 1) * HEAD_DIM] = total[k * groups + g : k * groups + g + 1, :]


def hand_on(*refs):
    n = len(refs) // 2
    sem = refs[-1]
    copies = [pltpu.make_async_copy(refs[k], refs[n + k], sem.at[k]) for k in range(n)]
    for c in copies:
        c.start()
    for c in copies:
        c.wait()


def solution(mesh):
    nz, nx = mesh.shape["sample"], mesh.shape["fsdp"]

    def shards(queries, comp_k, comp_v, prompt_k, prompt_v, output_grad, lengths):
        count, width = queries.shape[2:]
        kv_width = comp_k.shape[3]
        groups = kv_width // HEAD_DIM
        heads = width // HEAD_DIM
        wide = heads // groups * count
        key_count = nz * nx
        reach = nz // 4
        blocks = nx + 1
        anywhere = pl.BlockSpec(memory_space=pl.ANY)
        vmem = pl.BlockSpec(memory_space=pltpu.VMEM)
        smem = pl.BlockSpec(memory_space=pltpu.SMEM)
        dma = pltpu.SemaphoreType.DMA
        one = jax.ShapeDtypeStruct
        results = pl.pallas_call(
            functools.partial(kernel, nz, nx),
            out_shape=(
                pltpu.VMEM(queries.shape, BF16),
                pltpu.VMEM(queries.shape, BF16),
                pltpu.VMEM(comp_k.shape, F32),
                pltpu.VMEM(comp_k.shape, F32),
                pltpu.VMEM(prompt_k.shape, F32),
                pltpu.VMEM(prompt_k.shape, F32),
            ),
            in_specs=[anywhere] * 6 + [smem],
            out_specs=(vmem,) * 6,
            scratch_shapes=[
                pltpu.VMEM((heads * count, HEAD_DIM), BF16),
                pltpu.VMEM((heads * count, HEAD_DIM), BF16),
                pltpu.VMEM((heads * count // TILE, HEAD_DIM, TILE), BF16),
                pltpu.VMEM((heads * count // TILE, HEAD_DIM, TILE), BF16),
                pltpu.VMEM((blocks, 2, count, kv_width), BF16),
                pltpu.VMEM((blocks, 2, kv_width, count), BF16),
                pltpu.VMEM((nx, nz, 2 * groups, HEAD_DIM), BF16),
                pltpu.VMEM((key_count * 2 * groups, HEAD_DIM), F32),
                pltpu.VMEM((groups * nx, count, wide), F32),
                pltpu.VMEM((groups * nx, count, wide), F32),
                pltpu.VMEM((groups, HEAD_DIM, wide), F32),
                pltpu.VMEM((groups, HEAD_DIM, wide), F32),
                pltpu.VMEM((groups, 8, wide), F32),
                pltpu.VMEM((groups * nx, 1, wide), F32),
                pltpu.VMEM((count, wide), BF16),
                pltpu.VMEM((count, wide), BF16),
                pltpu.VMEM((groups, key_count, wide), BF16),
                pltpu.VMEM((groups, key_count, wide), BF16),
                pltpu.VMEM((nx, groups, 2, count, HEAD_DIM), BF16),
                pltpu.VMEM((nx - 1, groups, 2, count, HEAD_DIM), BF16),
                pltpu.VMEM((groups, 2, count, HEAD_DIM), F32),
                pltpu.VMEM((groups, nx, 2, nz, HEAD_DIM), BF16),
                pltpu.VMEM((groups, 2, nz, HEAD_DIM), F32),
                pltpu.VMEM((groups, nx, 2, nz, HEAD_DIM), BF16),
                pltpu.VMEM((nz * 2 * groups, HEAD_DIM), F32),
                pltpu.VMEM((nz, 2 * groups, HEAD_DIM), BF16),
                pltpu.VMEM((nz, 2 * groups, HEAD_DIM), BF16),
                pltpu.VMEM((2 * groups, HEAD_DIM), F32),
                pltpu.VMEM((2, *prompt_k.shape), BF16),
                dma((2, groups)),
                dma((2,)),
                dma((2,)),
                dma((2 * reach,)),
                dma((2 * reach,)),
                dma((2, reach)),
                dma((2, reach)),
                dma((6, nx - 1)),
                dma((6, nx - 1)),
                dma((2, nx - 1)),
                dma((2, nx - 1)),
                dma((groups, nx - 1)),
                dma((groups, nx - 1)),
                dma,
                dma,
                dma((nx, groups)),
                dma((nx - 1, groups)),
            ],
            compiler_params=pltpu.CompilerParams(
                collective_id=0, has_side_effects=True, vmem_limit_bytes=58 * 2**20
            ),
            name="attend",
        )(queries, comp_k, comp_v, prompt_k, prompt_v, output_grad, lengths)
        n = len(results)
        return pl.pallas_call(
            hand_on,
            out_shape=tuple(one(r.shape, r.dtype) for r in results),
            in_specs=[vmem] * n,
            out_specs=(anywhere,) * n,
            scratch_shapes=[dma((n,))],
            compiler_params=pltpu.CompilerParams(vmem_limit_bytes=2**20),
            name="hand_on",
        )(*(pltpu.with_memory_space_constraint(r, pltpu.VMEM) for r in results))

    rows = P(("groups", "prompt"), "sample", "fsdp", None)
    prompt_rows = P(("groups", "prompt"), ("sample", "fsdp"), None)
    return jax.shard_map(
        shards,
        mesh=mesh,
        in_specs=(rows, rows, rows, prompt_rows, prompt_rows, rows, P(("groups", "prompt"), "sample")),
        out_specs=(rows, rows, rows, rows, prompt_rows, prompt_rows),
        check_vma=False,
    )
```

```python
import functools
import math

import jax
import jax.numpy as jnp
from jax import lax
from jax.experimental import pallas as pl
from jax.experimental.pallas import tpu as pltpu
from jax.sharding import PartitionSpec as P

HEAD_DIM = 128
TILE = 256
MESH = pl.DeviceIdType.MESH
F32 = jnp.float32
BF16 = jnp.bfloat16


def dot(a, b):
    return jnp.dot(a, b, preferred_element_type=F32)


def kernel(
    nz,
    nx,
    queries,
    comp_k,
    comp_v,
    prompt_k,
    prompt_v,
    out_grad,
    lengths,
    out,
    query_grad,
    comp_k_grad,
    comp_v_grad,
    prompt_k_grad,
    prompt_v_grad,
    q_s,
    g_s,
    qt_s,
    gt_s,
    kv,
    kvt,
    rows,
    rows32,
    e_s,
    dp_s,
    o_s,
    dq_s,
    stat,
    blockmax,
    p_half,
    ds_half,
    pp_s,
    dsp_s,
    csend,
    crecv,
    cown,
    cterm,
    xsend,
    xown,
    xrecv,
    zf,
    zsend,
    zrecv,
    pstage,
    pin,
    in_sem,
    kvin_sem,
    pin_sem,
    r1_send,
    r1_recv,
    r2_send,
    r2_recv,
    rx_send,
    rx_recv,
    kv_send,
    kv_recv,
    x_send,
    x_recv,
    z_send,
    z_recv,
    c_send,
    c_recv,
):
    z = lax.axis_index("sample")
    x = lax.axis_index("fsdp")
    count = comp_k.shape[2]
    groups = comp_k.shape[3] // HEAD_DIM
    heads = queries.shape[3] // HEAD_DIM
    share = heads // groups
    wide = share * count
    tiles = wide // TILE
    reach = nz // 4
    scale = HEAD_DIM**-0.5
    fold = scale * math.log2(math.e)
    last = nx
    key_count = nz * nx

    def at_z(d):
        return {"sample": lax.rem(z + (d + nz) % nz, nz)}

    def at_x(d):
        return {"fsdp": lax.rem(x + d, nx)}

    def remote(src, dst, send, recv, to):
        return pltpu.make_async_remote_copy(
            src_ref=src, dst_ref=dst, send_sem=send, recv_sem=recv, device_id=to, device_id_type=MESH
        )

    barrier = pltpu.get_barrier_semaphore()
    near = [d for d in range(1, reach + 1)] + [-d for d in range(1, reach + 1)]
    for d in near:
        pl.semaphore_signal(barrier, inc=1, device_id=at_z(d), device_id_type=MESH)
    for d in range(1, nx):
        pl.semaphore_signal(barrier, inc=1, device_id=at_x(d), device_id_type=MESH)

    own_kv = [
        pltpu.make_async_copy(comp_k.at[0, 0], kv.at[x, 0], kvin_sem.at[0]),
        pltpu.make_async_copy(comp_v.at[0, 0], kv.at[x, 1], kvin_sem.at[1]),
    ]
    own_rows = [
        pltpu.make_async_copy(prompt_k, pin.at[0], pin_sem.at[0]),
        pltpu.make_async_copy(prompt_v, pin.at[1], pin_sem.at[1]),
    ]
    for c in own_rows + own_kv:
        c.start()

    @pl.loop(0, groups)
    def _(g):
        for h in range(share):
            head = g * share + h
            cols = pl.ds(pl.multiple_of(head * HEAD_DIM, HEAD_DIM), HEAD_DIM)
            dst = pl.ds(pl.multiple_of(head * count, count), count)
            pltpu.make_async_copy(queries.at[0, 0, :, cols], q_s.at[dst], in_sem.at[0, g]).start()
            pltpu.make_async_copy(out_grad.at[0, 0, :, cols], g_s.at[dst], in_sem.at[1, g]).start()

    for k in range(2):
        own_rows[k].wait()
        row = pin[k, 0].astype(F32)
        for g in range(groups):
            pstage[k * groups + g : k * groups + g + 1, :] = row[:, g * HEAD_DIM : (g + 1) * HEAD_DIM]
    rows[0, 0] = pstage[...].astype(BF16)

    def turn(b, begin, end):
        for part in range(2):
            for g in range(begin, end):
                cols = slice(g * HEAD_DIM, (g + 1) * HEAD_DIM)
                kvt[b, part, cols, :] = kv[b, part, :, cols].astype(F32).T.astype(BF16)

    def forward(b, g, first):
        cols = pl.ds(pl.multiple_of(g * HEAD_DIM, HEAD_DIM), HEAD_DIM)
        keys = kv[b, 0, :, cols]
        values = kv[b, 1, :, cols]
        values_t = kvt[b, 1, cols, :]
        slot = g * nx + b
        for t in range(tiles):
            at = slice(t * TILE, (t + 1) * TILE)
            s = dot(keys, qt_s[g * tiles + t])
            if first:
                key = lax.broadcasted_iota(jnp.int32, s.shape, 0)
                token = lax.broadcasted_iota(jnp.int32, s.shape, 1) % count
                s = jnp.where(key <= token, s, -1e30)
            top = jnp.max(s, axis=0, keepdims=True)
            if not first:
                before = stat[g, 0:1, at]
                top = jnp.maximum(top, before)
            e = jnp.exp2((s - top) * fold)
            total = jnp.sum(e, axis=0, keepdims=True)
            dp = dot(values, gt_s[g * tiles + t])
            mean = jnp.sum(e * dp, axis=0, keepdims=True)
            o = dot(values_t, e.astype(BF16))
            if not first:
                old = jnp.exp2((before - top) * fold)
                total += old * stat[g, 1:2, at]
                mean += old * stat[g, 2:3, at]
                o += old * o_s[g, :, at]
            stat[g, 0:1, at] = top
            stat[g, 1:2, at] = total
            stat[g, 2:3, at] = mean
            o_s[g, :, at] = o
            e_s[slot, :, at] = e
            dp_s[slot, :, at] = dp
            blockmax[slot, 0:1, at] = top

    def backward(b, g, first):
        cols = pl.ds(pl.multiple_of(g * HEAD_DIM, HEAD_DIM), HEAD_DIM)
        keys_t = kvt[b, 0, cols, :]
        slot = g * nx + b
        for t in range(tiles):
            at = slice(t * TILE, (t + 1) * TILE)
            factor = jnp.exp2((blockmax[slot, 0:1, at] - stat[g, 0:1, at]) * fold) * stat[g, 1:2, at]
            p = e_s[slot, :, at] * factor
            ds = (p * (dp_s[slot, :, at] - stat[g, 2:3, at])).astype(BF16)
            p_half[:, at] = p.astype(BF16)
            ds_half[:, at] = ds
            dq = dot(keys_t, ds)
            if first:
                dq += dot(kvt[last, 0, cols, :], dsp_s[g, :, at])
                dq_s[g, :, at] = dq
            else:
                dq_s[g, :, at] += dq
        src = pl.ds(pl.multiple_of(g * wide, wide), wide)
        return dot(ds_half[...], q_s[src, :]) * scale, dot(p_half[...], g_s[src, :])

    def flush(source, target, g):
        for t in range(tiles):
            block = source(slice(t * TILE, (t + 1) * TILE)).T.astype(BF16)
            for h in range(TILE // count):
                head = g * share + t * (TILE // count) + h
                cols = pl.ds(pl.multiple_of(head * HEAD_DIM, HEAD_DIM), HEAD_DIM)
                target[0, 0, :, cols] = block[h * count : (h + 1) * count]

    pl.semaphore_wait(barrier, len(near) + nx - 1)

    first_leg = {
        d: remote(
            rows.at[0, 0], rows.at[0, (nz - d) % nz], r1_send.at[n], r1_recv.at[n], at_z(d)
        )
        for n, d in enumerate(near)
    }
    for d in sorted(near, key=abs, reverse=True):
        first_leg[d].start()

    middle = groups // 2

    def kv_copy(half, b, kind, to):
        cols = pl.ds(half * middle * HEAD_DIM, middle * HEAD_DIM)
        block = kv.at[b, :, :, cols]
        return remote(block, block, kv_send.at[half, kind], kv_recv.at[half, b], {"fsdp": to})

    own_sends = [(p, half, p, 0, p + 1) for half in range(2) for p in range(nx - 1)]
    own_sends += [(0, half, 0, 1, nx - 1) for half in range(2)] + [(1, 1, 1, 1, 0)]
    pass_first = [(1, 0, 0, 2, 2), (2, 0, 1, 2, 3)]
    pass_second = [(1, 1, 0, 2, 2), (0, 1, 1, 2, 3)]

    def own_send(entry):
        p, half, b, kind, to = entry

        @pl.when(x == p)
        def _():
            kv_copy(half, b, kind, to).start()

    def pass_on(entry):
        p, half, b, kind, to = entry

        @pl.when(x == p)
        def _():
            c = kv_copy(half, b, kind, to)
            c.wait_recv()
            c.start()

    for c in own_kv:
        c.wait()
    for entry in own_sends:
        own_send(entry)

    turn(x, 0, groups)
    token = lax.broadcasted_iota(jnp.int32, (count, HEAD_DIM), 0) + x * count
    length = jnp.full((count, HEAD_DIM), lengths[0, 0], jnp.int32)
    weight = jnp.where(token < length, F32(count * nx) / length.astype(F32), 0.0)

    @pl.loop(0, groups, unroll=2)
    def _(g):
        src = pl.ds(pl.multiple_of(g * wide, wide), wide)
        pltpu.make_async_copy(q_s.at[src], q_s.at[src], in_sem.at[0, g]).wait()
        pltpu.make_async_copy(g_s.at[src], g_s.at[src], in_sem.at[1, g]).wait()
        for h in range(share):
            at = pl.ds(pl.multiple_of((g * share + h) * count, count), count)
            g_s[at, :] = (g_s[at, :].astype(F32) * weight).astype(BF16)
        for t in range(tiles):
            src = pl.ds(pl.multiple_of(g * wide + t * TILE, TILE), TILE)
            qt_s[g * tiles + t] = q_s[src, :].astype(F32).T.astype(BF16)
            gt_s[g * tiles + t] = g_s[src, :].astype(F32).T.astype(BF16)
        forward(x, g, True)

    for entry in pass_first:
        pass_on(entry)

    second_leg = []
    for e in range(1, reach + 1):
        first_leg[-e].wait_recv()
        c = remote(
            rows.at[0, e], rows.at[0, reach + e], r2_send.at[0, e - 1], r2_recv.at[0, e - 1], at_z(-reach)
        )
        c.start()
        second_leg.append(c)
        first_leg[e].wait_recv()
        if e < reach:
            c = remote(
                rows.at[0, nz - e],
                rows.at[0, nz - reach - e],
                r2_send.at[1, e - 1],
                r2_recv.at[1, e - 1],
                at_z(reach),
            )
            c.start()
            second_leg.append(c)

    def to_columns(part, begin, end):
        return [
            remote(
                rows.at[0, begin:end],
                rows.at[nx - d, begin:end],
                rx_send.at[part, d - 1],
                rx_recv.at[part, d - 1],
                at_x(d),
            )
            for d in range(1, nx)
        ]

    column_legs = to_columns(0, 0, reach + 1) + to_columns(1, nz - reach, nz)
    for c in column_legs:
        c.start()

    def earlier(half):
        @pl.loop(0, nx - 1)
        def _(n):
            d = lax.rem(n + nx - 2, nx - 1) + 1

            @pl.when(d <= x)
            def _():
                b = x - d
                passed = (x == 1) if half else (x == 1) | ((x == 2) & (b == 1))

                @pl.when(jnp.logical_not(passed))
                def _():
                    kv_copy(half, b, 0, lax.rem(x + 1, nx)).wait_recv()

                turn(b, half * middle, (half + 1) * middle)

                @pl.loop(half * middle, (half + 1) * middle, unroll=2)
                def _(g):
                    forward(b, g, False)

    for entry in pass_second:
        pass_on(entry)

    earlier(0)

    ahead, behind = second_leg[0::2], second_leg[1::2]
    ahead += behind[reach - 1 :]
    behind = behind[: reach - 1]
    half = reach // 2
    pieces = [
        (ahead[:half], reach + 1, reach + 1 + half),
        (behind[:half], nz - reach - half, nz - reach),
        (ahead[half:], reach + 1 + half, 2 * reach + 1),
        (behind[half:], 2 * reach + 1, nz - reach - half),
    ]
    for n, (arrivals, begin, end) in enumerate(pieces):
        for c in arrivals:
            c.wait_recv()
        if end > begin:
            legs = to_columns(2 + n, begin, end)
            for c in legs:
                c.start()
            column_legs += legs

    earlier(1)

    for c in column_legs:
        c.wait_recv()

    for d in range(nx):
        part_rows = nz * 2 * groups
        rows32[d * part_rows : (d + 1) * part_rows, :] = rows[d].astype(F32).reshape(part_rows, HEAD_DIM)
    for part in range(2):
        for g in range(groups):
            cols = slice(g * HEAD_DIM, (g + 1) * HEAD_DIM)
            block = rows32[pl.ds(part * groups + g, key_count, stride=2 * groups), :]
            kv[last, part, :, cols] = block.astype(BF16)
            kvt[last, part, cols, :] = block.T.astype(BF16)

    def x_copy(g, d):
        return remote(
            xsend.at[g, d], xrecv.at[g, nx - d], x_send.at[g, d - 1], x_recv.at[g, d - 1], at_x(d)
        )

    @pl.loop(0, groups, unroll=2)
    def _(g):
        cols = pl.ds(pl.multiple_of(g * HEAD_DIM, HEAD_DIM), HEAD_DIM)
        keys = kv[last, 0, :, cols]
        values = kv[last, 1, :, cols]
        for t in range(tiles):
            at = slice(t * TILE, (t + 1) * TILE)
            s = dot(keys, qt_s[g * tiles + t])
            before = stat[g, 0:1, at]
            top = jnp.maximum(jnp.max(s, axis=0, keepdims=True), before)
            e = jnp.exp2((s - top) * fold)
            old = jnp.exp2((before - top) * fold)
            inverse = 1.0 / (old * stat[g, 1:2, at] + jnp.sum(e, axis=0, keepdims=True))
            dp = dot(values, gt_s[g * tiles + t])
            p = e * inverse
            mean = old * inverse * stat[g, 2:3, at] + jnp.sum(p * dp, axis=0, keepdims=True)
            pp_s[g, :, at] = p.astype(BF16)
            dsp_s[g, :, at] = (p * (dp - mean)).astype(BF16)
            stat[g, 0:1, at] = top
            stat[g, 1:2, at] = inverse
            stat[g, 2:3, at] = mean
            stat[g, 3:4, at] = old * inverse
        src = pl.ds(pl.multiple_of(g * wide, wide), wide)
        both = dot(dsp_s[g], q_s[src, :]) * scale, dot(pp_s[g], g_s[src, :])
        for part in range(2):
            xown[g, part] = both[part][:nz]
            for d in range(1, nx):
                xsend[g, d, part] = both[part][d * nz : (d + 1) * nz].astype(BF16)
        for d in range(1, nx):
            x_copy(g, d).start()

    def c_copy(b, g, slot, to):
        return remote(csend.at[b, g], crecv.at[slot, g], c_send.at[b, g], c_recv.at[slot, g], {"fsdp": to})

    @pl.loop(0, groups, unroll=2)
    def _(g):
        both = backward(x, g, True)
        for part in range(2):
            cown[g, part] = both[part]

    def earlier_backward(n):
        edge = x == nx - 1
        b = lax.rem(n + edge.astype(jnp.int32), nx - 1)
        short = edge & (b == 0)
        more = jnp.logical_not(edge) & ((b > 0) | (x < nx - 2))
        slot = jnp.where(short, nx - 1, b)
        to = jnp.where(short, 0, x - 1)

        @pl.loop(0, groups // 2)
        def _(pair):
            for k in range(2):
                both = backward(b, 2 * pair + k, False)
                for part in range(2):
                    cterm[k, part] = both[part]
            for k in range(2):
                g = 2 * pair + k

                @pl.when(more)
                def _(g=g, k=k):
                    c_copy(b, g, b, to).wait_recv()
                    for part in range(2):
                        cterm[k, part] += crecv[b, g, part].astype(F32)

                for part in range(2):
                    csend[b, g, part] = cterm[k, part].astype(BF16)
                c_copy(b, g, slot, to).start()

    for g in range(groups):
        for d in range(1, nx):
            x_copy(g, d).wait_recv()
    for g in range(groups):
        for part in range(2):
            total = xown[g, part]
            for d in range(1, nx):
                total += xrecv[g, d, part].astype(F32)
            zf[pl.ds(part * groups + g, nz, stride=2 * groups), :] = total
    zsend[...] = zf[...].reshape(nz, 2 * groups, HEAD_DIM).astype(BF16)

    def z_copy(s):
        return remote(zsend.at[s], zrecv.at[nz - s], z_send, z_recv, at_z(s))

    for s in sorted(range(1, nz), key=lambda s: min(s, nz - s), reverse=True):
        z_copy(s).start()

    @pl.loop(0, jnp.minimum(x, 1))
    def _(n):
        earlier_backward(n)

    @pl.loop(0, groups)
    def _(g):
        cols = pl.ds(pl.multiple_of(g * HEAD_DIM, HEAD_DIM), HEAD_DIM)
        values_t = kvt[last, 1, cols, :]
        flush(
            lambda at: o_s[g, :, at] * stat[g, 3:4, at] + dot(values_t, pp_s[g, :, at]),
            out,
            g,
        )

    @pl.loop(1, x)
    def _(n):
        earlier_backward(n)

    @pl.loop(0, groups)
    def _(g):
        flush(lambda at: dq_s[g, :, at] * scale, query_grad, g)

    def collect(slot):
        for g in range(groups):
            c_copy(0, g, slot, lax.rem(x + 1, nx)).wait_recv()
            for part in range(2):
                cown[g, part] += crecv[slot, g, part].astype(F32)

    @pl.when((x < nx - 1) & ((x > 0) | (x < nx - 2)))
    def _():
        collect(x)

    @pl.when(x == 0)
    def _():
        collect(nx - 1)

    for part, ref in enumerate((comp_k_grad, comp_v_grad)):
        for g in range(groups):
            ref[0, 0, :, g * HEAD_DIM : (g + 1) * HEAD_DIM] = cown[g, part]

    for entry in own_sends + pass_first + pass_second:

        @pl.when(x == entry[0])
        def _(entry=entry):
            kv_copy(*entry[1:]).wait_send()

    for c in list(first_leg.values()) + second_leg + column_legs:
        c.wait_send()
    for d in range(1, nx):

        for g in range(groups):
            x_copy(g, d).wait_send()
    pltpu.make_async_copy(zsend.at[1:nz], zsend.at[1:nz], z_send).wait()

    @pl.loop(0, x)
    def _(b):
        for g in range(groups):
            c_copy(b, g, 0, lax.rem(x + 1, nx)).wait_send()

    pltpu.make_async_copy(zrecv.at[1:nz], zrecv.at[1:nz], z_recv).wait()
    total = zf[: 2 * groups, :]
    for s in range(1, nz):
        total += zrecv[s].astype(F32)
    for k, ref in enumerate((prompt_k_grad, prompt_v_grad)):
        for g in range(groups):
            ref[0, :, g * HEAD_DIM : (g + 1) * HEAD_DIM] = total[k * groups + g : k * groups + g + 1, :]


def hand_on(*refs):
    n = len(refs) // 2
    sem = refs[-1]
    copies = [pltpu.make_async_copy(refs[k], refs[n + k], sem.at[k]) for k in range(n)]
    for c in copies:
        c.start()
    for c in copies:
        c.wait()


def solution(mesh):
    nz, nx = mesh.shape["sample"], mesh.shape["fsdp"]

    def shards(queries, comp_k, comp_v, prompt_k, prompt_v, output_grad, lengths):
        count, width = queries.shape[2:]
        kv_width = comp_k.shape[3]
        groups = kv_width // HEAD_DIM
        heads = width // HEAD_DIM
        wide = heads // groups * count
        key_count = nz * nx
        reach = nz // 4
        blocks = nx + 1
        anywhere = pl.BlockSpec(memory_space=pl.ANY)
        vmem = pl.BlockSpec(memory_space=pltpu.VMEM)
        smem = pl.BlockSpec(memory_space=pltpu.SMEM)
        dma = pltpu.SemaphoreType.DMA
        one = jax.ShapeDtypeStruct
        results = pl.pallas_call(
            functools.partial(kernel, nz, nx),
            out_shape=(
                pltpu.VMEM(queries.shape, BF16),
                pltpu.VMEM(queries.shape, BF16),
                pltpu.VMEM(comp_k.shape, F32),
                pltpu.VMEM(comp_k.shape, F32),
                pltpu.VMEM(prompt_k.shape, F32),
                pltpu.VMEM(prompt_k.shape, F32),
            ),
            in_specs=[anywhere] * 6 + [smem],
            out_specs=(vmem,) * 6,
            scratch_shapes=[
                pltpu.VMEM((heads * count, HEAD_DIM), BF16),
                pltpu.VMEM((heads * count, HEAD_DIM), BF16),
                pltpu.VMEM((heads * count // TILE, HEAD_DIM, TILE), BF16),
                pltpu.VMEM((heads * count // TILE, HEAD_DIM, TILE), BF16),
                pltpu.VMEM((blocks, 2, count, kv_width), BF16),
                pltpu.VMEM((blocks, 2, kv_width, count), BF16),
                pltpu.VMEM((nx, nz, 2 * groups, HEAD_DIM), BF16),
                pltpu.VMEM((key_count * 2 * groups, HEAD_DIM), F32),
                pltpu.VMEM((groups * nx, count, wide), F32),
                pltpu.VMEM((groups * nx, count, wide), F32),
                pltpu.VMEM((groups, HEAD_DIM, wide), F32),
                pltpu.VMEM((groups, HEAD_DIM, wide), F32),
                pltpu.VMEM((groups, 8, wide), F32),
                pltpu.VMEM((groups * nx, 1, wide), F32),
                pltpu.VMEM((count, wide), BF16),
                pltpu.VMEM((count, wide), BF16),
                pltpu.VMEM((groups, key_count, wide), BF16),
                pltpu.VMEM((groups, key_count, wide), BF16),
                pltpu.VMEM((nx, groups, 2, count, HEAD_DIM), BF16),
                pltpu.VMEM((nx, groups, 2, count, HEAD_DIM), BF16),
                pltpu.VMEM((groups, 2, count, HEAD_DIM), F32),
                pltpu.VMEM((2, 2, count, HEAD_DIM), F32),
                pltpu.VMEM((groups, nx, 2, nz, HEAD_DIM), BF16),
                pltpu.VMEM((groups, 2, nz, HEAD_DIM), F32),
                pltpu.VMEM((groups, nx, 2, nz, HEAD_DIM), BF16),
                pltpu.VMEM((nz * 2 * groups, HEAD_DIM), F32),
                pltpu.VMEM((nz, 2 * groups, HEAD_DIM), BF16),
                pltpu.VMEM((nz, 2 * groups, HEAD_DIM), BF16),
                pltpu.VMEM((2 * groups, HEAD_DIM), F32),
                pltpu.VMEM((2, *prompt_k.shape), BF16),
                dma((2, groups)),
                dma((2,)),
                dma((2,)),
                dma((2 * reach,)),
                dma((2 * reach,)),
                dma((2, reach)),
                dma((2, reach)),
                dma((6, nx - 1)),
                dma((6, nx - 1)),
                dma((2, 3)),
                dma((2, nx)),
                dma((groups, nx - 1)),
                dma((groups, nx - 1)),
                dma,
                dma,
                dma((nx, groups)),
                dma((nx, groups)),
            ],
            compiler_params=pltpu.CompilerParams(
                collective_id=0, has_side_effects=True, vmem_limit_bytes=58 * 2**20
            ),
            name="attend",
        )(queries, comp_k, comp_v, prompt_k, prompt_v, output_grad, lengths)
        n = len(results)
        return pl.pallas_call(
            hand_on,
            out_shape=tuple(one(r.shape, r.dtype) for r in results),
            in_specs=[vmem] * n,
            out_specs=(anywhere,) * n,
            scratch_shapes=[dma((n,))],
            compiler_params=pltpu.CompilerParams(vmem_limit_bytes=2**20),
            name="hand_on",
        )(*(pltpu.with_memory_space_constraint(r, pltpu.VMEM) for r in results))

    rows = P(("groups", "prompt"), "sample", "fsdp", None)
    prompt_rows = P(("groups", "prompt"), ("sample", "fsdp"), None)
    return jax.shard_map(
        shards,
        mesh=mesh,
        in_specs=(rows, rows, rows, prompt_rows, prompt_rows, rows, P(("groups", "prompt"), "sample")),
        out_specs=(rows, rows, rows, rows, prompt_rows, prompt_rows),
        check_vma=False,
    )
```

```python
import functools
import math

import jax
import jax.numpy as jnp
from jax import lax
from jax.experimental import pallas as pl
from jax.experimental.pallas import tpu as pltpu
from jax.sharding import PartitionSpec as P

HEAD_DIM = 128
TILE = 256
MESH = pl.DeviceIdType.MESH
F32 = jnp.float32
BF16 = jnp.bfloat16


def dot(a, b):
    return jnp.dot(a, b, preferred_element_type=F32)


def kernel(
    nz,
    nx,
    queries,
    comp_k,
    comp_v,
    prompt_k,
    prompt_v,
    out_grad,
    lengths,
    out,
    query_grad,
    comp_k_grad,
    comp_v_grad,
    prompt_k_grad,
    prompt_v_grad,
    q_s,
    g_s,
    qt_s,
    gt_s,
    kv,
    kvt,
    rows,
    rows32,
    e_s,
    dp_s,
    o_s,
    dq_s,
    stat,
    blockmax,
    p_half,
    ds_half,
    pp_s,
    dsp_s,
    csend,
    crecv,
    cown,
    cterm,
    xsend,
    xown,
    xrecv,
    zf,
    zsend,
    zrecv,
    pstage,
    pin,
    in_sem,
    kvin_sem,
    pin_sem,
    r1_send,
    r1_recv,
    r2_send,
    r2_recv,
    rx_send,
    rx_recv,
    kv_send,
    kv_recv,
    x_send,
    x_recv,
    z_send,
    z_recv,
    c_send,
    c_recv,
):
    z = lax.axis_index("sample")
    x = lax.axis_index("fsdp")
    count = comp_k.shape[2]
    groups = comp_k.shape[3] // HEAD_DIM
    heads = queries.shape[3] // HEAD_DIM
    share = heads // groups
    wide = share * count
    tiles = wide // TILE
    reach = nz // 4
    scale = HEAD_DIM**-0.5
    fold = scale * math.log2(math.e)
    last = nx
    key_count = nz * nx

    def at_z(d):
        return {"sample": lax.rem(z + (d + nz) % nz, nz)}

    def at_x(d):
        return {"fsdp": lax.rem(x + d, nx)}

    def remote(src, dst, send, recv, to):
        return pltpu.make_async_remote_copy(
            src_ref=src, dst_ref=dst, send_sem=send, recv_sem=recv, device_id=to, device_id_type=MESH
        )

    barrier = pltpu.get_barrier_semaphore()
    near = [d for d in range(1, reach + 1)] + [-d for d in range(1, reach + 1)]
    for d in near:
        pl.semaphore_signal(barrier, inc=1, device_id=at_z(d), device_id_type=MESH)
    for d in range(1, nx):
        pl.semaphore_signal(barrier, inc=1, device_id=at_x(d), device_id_type=MESH)

    own_kv = [
        pltpu.make_async_copy(comp_k.at[0, 0], kv.at[x, 0], kvin_sem.at[0]),
        pltpu.make_async_copy(comp_v.at[0, 0], kv.at[x, 1], kvin_sem.at[1]),
    ]
    own_rows = [
        pltpu.make_async_copy(prompt_k, pin.at[0], pin_sem.at[0]),
        pltpu.make_async_copy(prompt_v, pin.at[1], pin_sem.at[1]),
    ]
    for c in own_rows + own_kv:
        c.start()

    @pl.loop(0, groups)
    def _(g):
        for h in range(share):
            head = g * share + h
            cols = pl.ds(pl.multiple_of(head * HEAD_DIM, HEAD_DIM), HEAD_DIM)
            dst = pl.ds(pl.multiple_of(head * count, count), count)
            pltpu.make_async_copy(queries.at[0, 0, :, cols], q_s.at[dst], in_sem.at[0, g]).start()
            pltpu.make_async_copy(out_grad.at[0, 0, :, cols], g_s.at[dst], in_sem.at[1, g]).start()

    for k in range(2):
        own_rows[k].wait()
        row = pin[k, 0].astype(F32)
        for g in range(groups):
            pstage[k * groups + g : k * groups + g + 1, :] = row[:, g * HEAD_DIM : (g + 1) * HEAD_DIM]
    rows[0, 0] = pstage[...].astype(BF16)

    def turn(b, begin, end):
        for part in range(2):
            for g in range(begin, end):
                cols = slice(g * HEAD_DIM, (g + 1) * HEAD_DIM)
                kvt[b, part, cols, :] = kv[b, part, :, cols].astype(F32).T.astype(BF16)

    def forward(b, g, first):
        cols = pl.ds(pl.multiple_of(g * HEAD_DIM, HEAD_DIM), HEAD_DIM)
        keys = kv[b, 0, :, cols]
        values = kv[b, 1, :, cols]
        values_t = kvt[b, 1, cols, :]
        slot = g * nx + b
        for t in range(tiles):
            at = slice(t * TILE, (t + 1) * TILE)
            s = dot(keys, qt_s[g * tiles + t])
            if first:
                key = lax.broadcasted_iota(jnp.int32, s.shape, 0)
                token = lax.broadcasted_iota(jnp.int32, s.shape, 1) % count
                s = jnp.where(key <= token, s, -1e30)
            top = jnp.max(s, axis=0, keepdims=True)
            if not first:
                before = stat[g, 0:1, at]
                top = jnp.maximum(top, before)
            e = jnp.exp2((s - top) * fold)
            total = jnp.sum(e, axis=0, keepdims=True)
            dp = dot(values, gt_s[g * tiles + t])
            mean = jnp.sum(e * dp, axis=0, keepdims=True)
            o = dot(values_t, e.astype(BF16))
            if not first:
                old = jnp.exp2((before - top) * fold)
                total += old * stat[g, 1:2, at]
                mean += old * stat[g, 2:3, at]
                o += old * o_s[g, :, at]
            stat[g, 0:1, at] = top
            stat[g, 1:2, at] = total
            stat[g, 2:3, at] = mean
            o_s[g, :, at] = o
            e_s[slot, :, at] = e
            dp_s[slot, :, at] = dp
            blockmax[slot, 0:1, at] = top

    def backward(b, g, first):
        cols = pl.ds(pl.multiple_of(g * HEAD_DIM, HEAD_DIM), HEAD_DIM)
        keys_t = kvt[b, 0, cols, :]
        slot = g * nx + b
        for t in range(tiles):
            at = slice(t * TILE, (t + 1) * TILE)
            factor = jnp.exp2((blockmax[slot, 0:1, at] - stat[g, 0:1, at]) * fold) * stat[g, 1:2, at]
            p = e_s[slot, :, at] * factor
            ds = (p * (dp_s[slot, :, at] - stat[g, 2:3, at])).astype(BF16)
            p_half[:, at] = p.astype(BF16)
            ds_half[:, at] = ds
            dq = dot(keys_t, ds)
            if first:
                dq += dot(kvt[last, 0, cols, :], dsp_s[g, :, at])
                dq_s[g, :, at] = dq
            else:
                dq_s[g, :, at] += dq
        src = pl.ds(pl.multiple_of(g * wide, wide), wide)
        return dot(ds_half[...], q_s[src, :]) * scale, dot(p_half[...], g_s[src, :])

    def flush(source, target, g):
        for t in range(tiles):
            block = source(slice(t * TILE, (t + 1) * TILE)).T.astype(BF16)
            for h in range(TILE // count):
                head = g * share + t * (TILE // count) + h
                cols = pl.ds(pl.multiple_of(head * HEAD_DIM, HEAD_DIM), HEAD_DIM)
                target[0, 0, :, cols] = block[h * count : (h + 1) * count]

    pl.semaphore_wait(barrier, len(near) + nx - 1)

    first_leg = {
        d: remote(
            rows.at[0, 0], rows.at[0, (nz - d) % nz], r1_send, r1_recv.at[n], at_z(d)
        )
        for n, d in enumerate(near)
    }
    for d in sorted(near, key=abs, reverse=True):
        first_leg[d].start()

    middle = groups // 2

    def kv_copy(half, b, kind, to):
        cols = pl.ds(half * middle * HEAD_DIM, middle * HEAD_DIM)
        block = kv.at[b, :, :, cols]
        return remote(block, block, kv_send.at[half, kind], kv_recv.at[half, b], {"fsdp": to})

    own_sends = [(p, half, p, 0, p + 1) for half in range(2) for p in range(nx - 1)]
    own_sends += [(0, half, 0, 1, nx - 1) for half in range(2)] + [(1, 1, 1, 1, 0)]
    pass_first = [(1, 0, 0, 2, 2), (2, 0, 1, 2, 3)]
    pass_second = [(1, 1, 0, 2, 2), (0, 1, 1, 2, 3)]

    def own_send(entry):
        p, half, b, kind, to = entry

        @pl.when(x == p)
        def _():
            kv_copy(half, b, kind, to).start()

    def pass_on(entry):
        p, half, b, kind, to = entry

        @pl.when(x == p)
        def _():
            c = kv_copy(half, b, kind, to)
            c.wait_recv()
            c.start()

    for c in own_kv:
        c.wait()
    for entry in own_sends:
        own_send(entry)

    turn(x, 0, groups)
    token = lax.broadcasted_iota(jnp.int32, (count, HEAD_DIM), 0) + x * count
    length = jnp.full((count, HEAD_DIM), lengths[0, 0], jnp.int32)
    weight = jnp.where(token < length, F32(count * nx) / length.astype(F32), 0.0)

    @pl.loop(0, groups, unroll=2)
    def _(g):
        src = pl.ds(pl.multiple_of(g * wide, wide), wide)
        pltpu.make_async_copy(q_s.at[src], q_s.at[src], in_sem.at[0, g]).wait()
        pltpu.make_async_copy(g_s.at[src], g_s.at[src], in_sem.at[1, g]).wait()
        for h in range(share):
            at = pl.ds(pl.multiple_of((g * share + h) * count, count), count)
            g_s[at, :] = (g_s[at, :].astype(F32) * weight).astype(BF16)
        for t in range(tiles):
            src = pl.ds(pl.multiple_of(g * wide + t * TILE, TILE), TILE)
            qt_s[g * tiles + t] = q_s[src, :].astype(F32).T.astype(BF16)
            gt_s[g * tiles + t] = g_s[src, :].astype(F32).T.astype(BF16)
        forward(x, g, True)

    for entry in pass_first:
        pass_on(entry)

    second_leg = []
    for e in range(1, reach + 1):
        first_leg[-e].wait_recv()
        c = remote(
            rows.at[0, e], rows.at[0, reach + e], r2_send, r2_recv.at[0, e - 1], at_z(-reach)
        )
        c.start()
        second_leg.append(c)
        first_leg[e].wait_recv()
        if e < reach:
            c = remote(
                rows.at[0, nz - e],
                rows.at[0, nz - reach - e],
                r2_send,
                r2_recv.at[1, e - 1],
                at_z(reach),
            )
            c.start()
            second_leg.append(c)

    def to_columns(begin, end):
        return [
            remote(
                rows.at[0, begin:end],
                rows.at[nx - d, begin:end],
                rx_send,
                rx_recv,
                at_x(d),
            )
            for d in range(1, nx)
        ]

    column_legs = to_columns(0, reach + 1) + to_columns(nz - reach, nz)
    for c in column_legs:
        c.start()

    def earlier(half):
        @pl.loop(0, nx - 1)
        def _(n):
            d = lax.rem(n + nx - 2, nx - 1) + 1

            @pl.when(d <= x)
            def _():
                b = x - d
                passed = (x == 1) if half else (x == 1) | ((x == 2) & (b == 1))

                @pl.when(jnp.logical_not(passed))
                def _():
                    kv_copy(half, b, 0, lax.rem(x + 1, nx)).wait_recv()

                turn(b, half * middle, (half + 1) * middle)

                @pl.loop(half * middle, (half + 1) * middle, unroll=2)
                def _(g):
                    forward(b, g, False)

    for entry in pass_second:
        pass_on(entry)

    earlier(0)

    ahead, behind = second_leg[0::2], second_leg[1::2]
    ahead += behind[reach - 1 :]
    behind = behind[: reach - 1]
    half = reach // 2
    pieces = [
        (ahead[:half], reach + 1, reach + 1 + half),
        (behind[:half], nz - reach - half, nz - reach),
        (ahead[half:], reach + 1 + half, 2 * reach + 1),
        (behind[half:], 2 * reach + 1, nz - reach - half),
    ]
    for arrivals, begin, end in pieces:
        for c in arrivals:
            c.wait_recv()
        if end > begin:
            for c in to_columns(begin, end):
                c.start()

    earlier(1)

    pltpu.make_async_copy(rows.at[1:nx], rows.at[1:nx], rx_recv).wait()

    for d in range(nx):
        part_rows = nz * 2 * groups
        rows32[d * part_rows : (d + 1) * part_rows, :] = rows[d].astype(F32).reshape(part_rows, HEAD_DIM)
    for part in range(2):
        for g in range(groups):
            cols = slice(g * HEAD_DIM, (g + 1) * HEAD_DIM)
            block = rows32[pl.ds(part * groups + g, key_count, stride=2 * groups), :]
            kv[last, part, :, cols] = block.astype(BF16)
            kvt[last, part, cols, :] = block.T.astype(BF16)

    def x_copy(g, d):
        return remote(
            xsend.at[g, d], xrecv.at[g, nx - d], x_send, x_recv, at_x(d)
        )

    @pl.loop(0, groups, unroll=groups)
    def _(g):
        cols = pl.ds(pl.multiple_of(g * HEAD_DIM, HEAD_DIM), HEAD_DIM)
        keys = kv[last, 0, :, cols]
        values = kv[last, 1, :, cols]
        for t in range(tiles):
            at = slice(t * TILE, (t + 1) * TILE)
            s = dot(keys, qt_s[g * tiles + t])
            before = stat[g, 0:1, at]
            top = jnp.maximum(jnp.max(s, axis=0, keepdims=True), before)
            e = jnp.exp2((s - top) * fold)
            old = jnp.exp2((before - top) * fold)
            inverse = 1.0 / (old * stat[g, 1:2, at] + jnp.sum(e, axis=0, keepdims=True))
            dp = dot(values, gt_s[g * tiles + t])
            p = e * inverse
            mean = old * inverse * stat[g, 2:3, at] + jnp.sum(p * dp, axis=0, keepdims=True)
            pp_s[g, :, at] = p.astype(BF16)
            dsp_s[g, :, at] = (p * (dp - mean)).astype(BF16)
            stat[g, 0:1, at] = top
            stat[g, 1:2, at] = inverse
            stat[g, 2:3, at] = mean
            stat[g, 3:4, at] = old * inverse
        src = pl.ds(pl.multiple_of(g * wide, wide), wide)
        both = dot(dsp_s[g], q_s[src, :]) * scale, dot(pp_s[g], g_s[src, :])
        for part in range(2):
            xown[g, part] = both[part][:nz]
            for d in range(1, nx):
                xsend[g, d, part] = both[part][d * nz : (d + 1) * nz].astype(BF16)
        for d in range(1, nx):
            x_copy(g, d).start()

    def c_copy(b, g, slot, to):
        return remote(csend.at[b, g], crecv.at[slot, g], c_send.at[b, g], c_recv.at[slot, g], {"fsdp": to})

    @pl.loop(0, groups, unroll=2)
    def _(g):
        both = backward(x, g, True)
        for part in range(2):
            cown[g, part] = both[part]

    def earlier_backward(n):
        edge = x == nx - 1
        b = lax.rem(n + edge.astype(jnp.int32), nx - 1)
        short = edge & (b == 0)
        more = jnp.logical_not(edge) & ((b > 0) | (x < nx - 2))
        slot = jnp.where(short, nx - 1, b)
        to = jnp.where(short, 0, x - 1)

        @pl.loop(0, groups // 2)
        def _(pair):
            for k in range(2):
                both = backward(b, 2 * pair + k, False)
                for part in range(2):
                    cterm[k, part] = both[part]
            for k in range(2):
                g = 2 * pair + k

                @pl.when(more)
                def _(g=g, k=k):
                    c_copy(b, g, b, to).wait_recv()
                    for part in range(2):
                        cterm[k, part] += crecv[b, g, part].astype(F32)

                for part in range(2):
                    csend[b, g, part] = cterm[k, part].astype(BF16)
                c_copy(b, g, slot, to).start()

    pltpu.make_async_copy(xrecv.at[:, 1:nx], xrecv.at[:, 1:nx], x_recv).wait()
    for g in range(groups):
        for part in range(2):
            total = xown[g, part]
            for d in range(1, nx):
                total += xrecv[g, d, part].astype(F32)
            zf[pl.ds(part * groups + g, nz, stride=2 * groups), :] = total
    zsend[...] = zf[...].reshape(nz, 2 * groups, HEAD_DIM).astype(BF16)

    def z_copy(s):
        return remote(zsend.at[s], zrecv.at[nz - s], z_send, z_recv, at_z(s))

    for s in sorted(range(1, nz), key=lambda s: min(s, nz - s), reverse=True):
        z_copy(s).start()

    @pl.loop(0, jnp.minimum(x, 1))
    def _(n):
        earlier_backward(n)

    @pl.loop(0, groups)
    def _(g):
        cols = pl.ds(pl.multiple_of(g * HEAD_DIM, HEAD_DIM), HEAD_DIM)
        values_t = kvt[last, 1, cols, :]
        flush(
            lambda at: o_s[g, :, at] * stat[g, 3:4, at] + dot(values_t, pp_s[g, :, at]),
            out,
            g,
        )

    @pl.loop(1, x)
    def _(n):
        earlier_backward(n)

    @pl.loop(0, groups)
    def _(g):
        flush(lambda at: dq_s[g, :, at] * scale, query_grad, g)

    def collect(slot):
        for g in range(groups):
            c_copy(0, g, slot, lax.rem(x + 1, nx)).wait_recv()
            for part in range(2):
                cown[g, part] += crecv[slot, g, part].astype(F32)

    @pl.when((x < nx - 1) & ((x > 0) | (x < nx - 2)))
    def _():
        collect(x)

    @pl.when(x == 0)
    def _():
        collect(nx - 1)

    for part, ref in enumerate((comp_k_grad, comp_v_grad)):
        for g in range(groups):
            ref[0, 0, :, g * HEAD_DIM : (g + 1) * HEAD_DIM] = cown[g, part]

    for entry in own_sends + pass_first + pass_second:

        @pl.when(x == entry[0])
        def _(entry=entry):
            kv_copy(*entry[1:]).wait_send()

    sent = rows.at[0, 0 : 2 * reach]
    pltpu.make_async_copy(sent, sent, r1_send).wait()
    sent = rows.at[0, 0 : 2 * reach - 1]
    pltpu.make_async_copy(sent, sent, r2_send).wait()
    pltpu.make_async_copy(rows.at[1:nx], rows.at[1:nx], rx_send).wait()
    pltpu.make_async_copy(xsend.at[:, 1:nx], xsend.at[:, 1:nx], x_send).wait()
    pltpu.make_async_copy(zsend.at[1:nz], zsend.at[1:nz], z_send).wait()

    @pl.loop(0, x)
    def _(b):
        for g in range(groups):
            c_copy(b, g, 0, lax.rem(x + 1, nx)).wait_send()

    pltpu.make_async_copy(zrecv.at[1:nz], zrecv.at[1:nz], z_recv).wait()
    total = zf[: 2 * groups, :]
    for s in range(1, nz):
        total += zrecv[s].astype(F32)
    for k, ref in enumerate((prompt_k_grad, prompt_v_grad)):
        for g in range(groups):
            ref[0, :, g * HEAD_DIM : (g + 1) * HEAD_DIM] = total[k * groups + g : k * groups + g + 1, :]


def hand_on(*refs):
    n = len(refs) // 2
    sem = refs[-1]
    copies = [pltpu.make_async_copy(refs[k], refs[n + k], sem.at[k]) for k in range(n)]
    for c in copies:
        c.start()
    for c in copies:
        c.wait()


def solution(mesh):
    nz, nx = mesh.shape["sample"], mesh.shape["fsdp"]

    def shards(queries, comp_k, comp_v, prompt_k, prompt_v, output_grad, lengths):
        count, width = queries.shape[2:]
        kv_width = comp_k.shape[3]
        groups = kv_width // HEAD_DIM
        heads = width // HEAD_DIM
        wide = heads // groups * count
        key_count = nz * nx
        reach = nz // 4
        blocks = nx + 1
        anywhere = pl.BlockSpec(memory_space=pl.ANY)
        vmem = pl.BlockSpec(memory_space=pltpu.VMEM)
        smem = pl.BlockSpec(memory_space=pltpu.SMEM)
        dma = pltpu.SemaphoreType.DMA
        one = jax.ShapeDtypeStruct
        results = pl.pallas_call(
            functools.partial(kernel, nz, nx),
            out_shape=(
                pltpu.VMEM(queries.shape, BF16),
                pltpu.VMEM(queries.shape, BF16),
                pltpu.VMEM(comp_k.shape, F32),
                pltpu.VMEM(comp_k.shape, F32),
                pltpu.VMEM(prompt_k.shape, F32),
                pltpu.VMEM(prompt_k.shape, F32),
            ),
            in_specs=[anywhere] * 6 + [smem],
            out_specs=(vmem,) * 6,
            scratch_shapes=[
                pltpu.VMEM((heads * count, HEAD_DIM), BF16),
                pltpu.VMEM((heads * count, HEAD_DIM), BF16),
                pltpu.VMEM((heads * count // TILE, HEAD_DIM, TILE), BF16),
                pltpu.VMEM((heads * count // TILE, HEAD_DIM, TILE), BF16),
                pltpu.VMEM((blocks, 2, count, kv_width), BF16),
                pltpu.VMEM((blocks, 2, kv_width, count), BF16),
                pltpu.VMEM((nx, nz, 2 * groups, HEAD_DIM), BF16),
                pltpu.VMEM((key_count * 2 * groups, HEAD_DIM), F32),
                pltpu.VMEM((groups * nx, count, wide), F32),
                pltpu.VMEM((groups * nx, count, wide), F32),
                pltpu.VMEM((groups, HEAD_DIM, wide), F32),
                pltpu.VMEM((groups, HEAD_DIM, wide), F32),
                pltpu.VMEM((groups, 8, wide), F32),
                pltpu.VMEM((groups * nx, 1, wide), F32),
                pltpu.VMEM((count, wide), BF16),
                pltpu.VMEM((count, wide), BF16),
                pltpu.VMEM((groups, key_count, wide), BF16),
                pltpu.VMEM((groups, key_count, wide), BF16),
                pltpu.VMEM((nx, groups, 2, count, HEAD_DIM), BF16),
                pltpu.VMEM((nx, groups, 2, count, HEAD_DIM), BF16),
                pltpu.VMEM((groups, 2, count, HEAD_DIM), F32),
                pltpu.VMEM((2, 2, count, HEAD_DIM), F32),
                pltpu.VMEM((groups, nx, 2, nz, HEAD_DIM), BF16),
                pltpu.VMEM((groups, 2, nz, HEAD_DIM), F32),
                pltpu.VMEM((groups, nx, 2, nz, HEAD_DIM), BF16),
                pltpu.VMEM((nz * 2 * groups, HEAD_DIM), F32),
                pltpu.VMEM((nz, 2 * groups, HEAD_DIM), BF16),
                pltpu.VMEM((nz, 2 * groups, HEAD_DIM), BF16),
                pltpu.VMEM((2 * groups, HEAD_DIM), F32),
                pltpu.VMEM((2, *prompt_k.shape), BF16),
                dma((2, groups)),
                dma((2,)),
                dma((2,)),
                dma,
                dma((2 * reach,)),
                dma,
                dma((2, reach)),
                dma,
                dma,
                dma((2, 3)),
                dma((2, nx)),
                dma,
                dma,
                dma,
                dma,
                dma((nx, groups)),
                dma((nx, groups)),
            ],
            compiler_params=pltpu.CompilerParams(
                collective_id=0, has_side_effects=True, vmem_limit_bytes=58 * 2**20
            ),
            name="attend",
        )(queries, comp_k, comp_v, prompt_k, prompt_v, output_grad, lengths)
        n = len(results)
        return pl.pallas_call(
            hand_on,
            out_shape=tuple(one(r.shape, r.dtype) for r in results),
            in_specs=[vmem] * n,
            out_specs=(anywhere,) * n,
            scratch_shapes=[dma((n,))],
            compiler_params=pltpu.CompilerParams(vmem_limit_bytes=2**20),
            name="hand_on",
        )(*(pltpu.with_memory_space_constraint(r, pltpu.VMEM) for r in results))

    rows = P(("groups", "prompt"), "sample", "fsdp", None)
    prompt_rows = P(("groups", "prompt"), ("sample", "fsdp"), None)
    return jax.shard_map(
        shards,
        mesh=mesh,
        in_specs=(rows, rows, rows, prompt_rows, prompt_rows, rows, P(("groups", "prompt"), "sample")),
        out_specs=(rows, rows, rows, rows, prompt_rows, prompt_rows),
        check_vma=False,
    )
```

```python
import functools
import math

import jax
import jax.numpy as jnp
from jax import lax
from jax.experimental import pallas as pl
from jax.experimental.pallas import tpu as pltpu
from jax.sharding import PartitionSpec as P

HEAD_DIM = 128
TILE = 256
MESH = pl.DeviceIdType.MESH
F32 = jnp.float32
BF16 = jnp.bfloat16


def dot(a, b):
    return jnp.dot(a, b, preferred_element_type=F32)


def kernel(
    nz,
    nx,
    queries,
    comp_k,
    comp_v,
    prompt_k,
    prompt_v,
    out_grad,
    lengths,
    out,
    query_grad,
    comp_k_grad,
    comp_v_grad,
    prompt_k_grad,
    prompt_v_grad,
    q_s,
    g_s,
    qt_s,
    gt_s,
    kv,
    kvt,
    rows,
    rows32,
    e_s,
    dp_s,
    o_s,
    dq_s,
    stat,
    blockmax,
    p_half,
    ds_half,
    pp_s,
    dsp_s,
    csend,
    crecv,
    cown,
    cterm,
    xsend,
    xown,
    xrecv,
    zf,
    zsend,
    zrecv,
    pstage,
    pin,
    in_sem,
    kvin_sem,
    pin_sem,
    r1_send,
    r1_recv,
    r2_send,
    r2_recv,
    rx_send,
    rx_recv,
    kv_send,
    kv_recv,
    x_send,
    x_recv,
    z_send,
    z_recv,
    c_send,
    c_recv,
):
    z = lax.axis_index("sample")
    x = lax.axis_index("fsdp")
    count = comp_k.shape[2]
    groups = comp_k.shape[3] // HEAD_DIM
    heads = queries.shape[3] // HEAD_DIM
    share = heads // groups
    wide = share * count
    tiles = wide // TILE
    reach = nz // 4
    scale = HEAD_DIM**-0.5
    fold = scale * math.log2(math.e)
    last = nx
    key_count = nz * nx

    def at_z(d):
        return {"sample": lax.rem(z + (d + nz) % nz, nz)}

    def at_x(d):
        return {"fsdp": lax.rem(x + d, nx)}

    def remote(src, dst, send, recv, to):
        return pltpu.make_async_remote_copy(
            src_ref=src, dst_ref=dst, send_sem=send, recv_sem=recv, device_id=to, device_id_type=MESH
        )

    barrier = pltpu.get_barrier_semaphore()
    near = [d for d in range(1, reach + 1)] + [-d for d in range(1, reach + 1)]
    for d in near:
        pl.semaphore_signal(barrier, inc=1, device_id=at_z(d), device_id_type=MESH)
    for d in range(1, nx):
        pl.semaphore_signal(barrier, inc=1, device_id=at_x(d), device_id_type=MESH)

    own_kv = [
        pltpu.make_async_copy(comp_k.at[0, 0], kv.at[x, 0], kvin_sem.at[0]),
        pltpu.make_async_copy(comp_v.at[0, 0], kv.at[x, 1], kvin_sem.at[1]),
    ]
    own_rows = [
        pltpu.make_async_copy(prompt_k, pin.at[0], pin_sem.at[0]),
        pltpu.make_async_copy(prompt_v, pin.at[1], pin_sem.at[1]),
    ]
    for c in own_rows + own_kv:
        c.start()

    @pl.loop(0, groups)
    def _(g):
        for h in range(share):
            head = g * share + h
            cols = pl.ds(pl.multiple_of(head * HEAD_DIM, HEAD_DIM), HEAD_DIM)
            dst = pl.ds(pl.multiple_of(head * count, count), count)
            pltpu.make_async_copy(queries.at[0, 0, :, cols], q_s.at[dst], in_sem.at[0, g]).start()
            pltpu.make_async_copy(out_grad.at[0, 0, :, cols], g_s.at[dst], in_sem.at[1, g]).start()

    for k in range(2):
        own_rows[k].wait()
        row = pin[k, 0].astype(F32)
        for g in range(groups):
            pstage[k * groups + g : k * groups + g + 1, :] = row[:, g * HEAD_DIM : (g + 1) * HEAD_DIM]
    rows[0, 0] = pstage[...].astype(BF16)

    def turn(b, begin, end):
        for part in range(2):
            for g in range(begin, end):
                cols = slice(g * HEAD_DIM, (g + 1) * HEAD_DIM)
                kvt[b, part, cols, :] = kv[b, part, :, cols].astype(F32).T.astype(BF16)

    def forward(b, g, first):
        cols = pl.ds(pl.multiple_of(g * HEAD_DIM, HEAD_DIM), HEAD_DIM)
        keys = kv[b, 0, :, cols]
        values = kv[b, 1, :, cols]
        values_t = kvt[b, 1, cols, :]
        slot = g * nx + b
        for t in range(tiles):
            at = slice(t * TILE, (t + 1) * TILE)
            s = dot(keys, qt_s[g * tiles + t])
            if first:
                key = lax.broadcasted_iota(jnp.int32, s.shape, 0)
                token = lax.broadcasted_iota(jnp.int32, s.shape, 1) % count
                s = jnp.where(key <= token, s, -1e30)
            top = jnp.max(s, axis=0, keepdims=True)
            if not first:
                before = stat[g, 0:1, at]
                top = jnp.maximum(top, before)
            e = jnp.exp2((s - top) * fold)
            total = jnp.sum(e, axis=0, keepdims=True)
            dp = dot(values, gt_s[g * tiles + t])
            mean = jnp.sum(e * dp, axis=0, keepdims=True)
            o = dot(values_t, e.astype(BF16))
            if not first:
                old = jnp.exp2((before - top) * fold)
                total += old * stat[g, 1:2, at]
                mean += old * stat[g, 2:3, at]
                o += old * o_s[g, :, at]
            stat[g, 0:1, at] = top
            stat[g, 1:2, at] = total
            stat[g, 2:3, at] = mean
            o_s[g, :, at] = o
            e_s[slot, :, at] = e
            dp_s[slot, :, at] = dp
            blockmax[slot, 0:1, at] = top

    def backward(b, g, first):
        cols = pl.ds(pl.multiple_of(g * HEAD_DIM, HEAD_DIM), HEAD_DIM)
        keys_t = kvt[b, 0, cols, :]
        slot = g * nx + b
        for t in range(tiles):
            at = slice(t * TILE, (t + 1) * TILE)
            factor = jnp.exp2((blockmax[slot, 0:1, at] - stat[g, 0:1, at]) * fold) * stat[g, 1:2, at]
            p = e_s[slot, :, at] * factor
            ds = (p * (dp_s[slot, :, at] - stat[g, 2:3, at])).astype(BF16)
            p_half[:, at] = p.astype(BF16)
            ds_half[:, at] = ds
            dq = dot(keys_t, ds)
            if first:
                dq += dot(kvt[last, 0, cols, :], dsp_s[g, :, at])
                dq_s[g, :, at] = dq
            else:
                dq_s[g, :, at] += dq
        src = pl.ds(pl.multiple_of(g * wide, wide), wide)
        return dot(ds_half[...], q_s[src, :]) * scale, dot(p_half[...], g_s[src, :])

    def flush(source, target, g):
        for t in range(tiles):
            block = source(slice(t * TILE, (t + 1) * TILE)).T.astype(BF16)
            for h in range(TILE // count):
                head = g * share + t * (TILE // count) + h
                cols = pl.ds(pl.multiple_of(head * HEAD_DIM, HEAD_DIM), HEAD_DIM)
                target[0, 0, :, cols] = block[h * count : (h + 1) * count]

    pl.semaphore_wait(barrier, len(near) + nx - 1)

    first_leg = {
        d: remote(
            rows.at[0, 0], rows.at[0, (nz - d) % nz], r1_send, r1_recv.at[n], at_z(d)
        )
        for n, d in enumerate(near)
    }
    for d in sorted(near, key=abs, reverse=True):
        first_leg[d].start()

    middle = groups // 2

    def kv_copy(half, b, kind, to):
        cols = pl.ds(half * middle * HEAD_DIM, middle * HEAD_DIM)
        block = kv.at[b, :, :, cols]
        return remote(block, block, kv_send.at[half, kind], kv_recv.at[half, b], {"fsdp": to})

    own_sends = [(p, half, p, 0, p + 1) for half in range(2) for p in range(nx - 1)]
    own_sends += [(0, half, 0, 1, nx - 1) for half in range(2)] + [(1, 1, 1, 1, 0)]
    pass_first = [(1, 0, 0, 2, 2), (2, 0, 1, 2, 3)]
    pass_second = [(1, 1, 0, 2, 2), (0, 1, 1, 2, 3)]

    def own_send(entry):
        p, half, b, kind, to = entry

        @pl.when(x == p)
        def _():
            kv_copy(half, b, kind, to).start()

    def pass_on(entry):
        p, half, b, kind, to = entry

        @pl.when(x == p)
        def _():
            c = kv_copy(half, b, kind, to)
            c.wait_recv()
            c.start()

    for c in own_kv:
        c.wait()
    for entry in own_sends:
        own_send(entry)

    turn(x, 0, groups)
    token = lax.broadcasted_iota(jnp.int32, (count, HEAD_DIM), 0) + x * count
    length = jnp.full((count, HEAD_DIM), lengths[0, 0], jnp.int32)
    weight = jnp.where(token < length, F32(count * nx) / length.astype(F32), 0.0)

    @pl.loop(0, groups, unroll=2)
    def _(g):
        src = pl.ds(pl.multiple_of(g * wide, wide), wide)
        pltpu.make_async_copy(q_s.at[src], q_s.at[src], in_sem.at[0, g]).wait()
        pltpu.make_async_copy(g_s.at[src], g_s.at[src], in_sem.at[1, g]).wait()
        for h in range(share):
            at = pl.ds(pl.multiple_of((g * share + h) * count, count), count)
            g_s[at, :] = (g_s[at, :].astype(F32) * weight).astype(BF16)
        for t in range(tiles):
            src = pl.ds(pl.multiple_of(g * wide + t * TILE, TILE), TILE)
            qt_s[g * tiles + t] = q_s[src, :].astype(F32).T.astype(BF16)
            gt_s[g * tiles + t] = g_s[src, :].astype(F32).T.astype(BF16)
        forward(x, g, True)

    for entry in pass_first:
        pass_on(entry)

    second_leg = []
    for e in range(1, reach + 1):
        first_leg[-e].wait_recv()
        c = remote(
            rows.at[0, e], rows.at[0, reach + e], r2_send, r2_recv.at[0, e - 1], at_z(-reach)
        )
        c.start()
        second_leg.append(c)
        first_leg[e].wait_recv()
        if e < reach:
            c = remote(
                rows.at[0, nz - e],
                rows.at[0, nz - reach - e],
                r2_send,
                r2_recv.at[1, e - 1],
                at_z(reach),
            )
            c.start()
            second_leg.append(c)

    def to_columns(begin, end):
        return [
            remote(
                rows.at[0, begin:end],
                rows.at[nx - d, begin:end],
                rx_send,
                rx_recv,
                at_x(d),
            )
            for d in range(1, nx)
        ]

    column_legs = to_columns(0, reach + 1) + to_columns(nz - reach, nz)
    for c in column_legs:
        c.start()

    def earlier(half):
        @pl.loop(0, nx - 1)
        def _(n):
            d = lax.rem(n + nx - 2, nx - 1) + 1

            @pl.when(d <= x)
            def _():
                b = x - d
                passed = (x == 1) if half else (x == 1) | ((x == 2) & (b == 1))

                @pl.when(jnp.logical_not(passed))
                def _():
                    kv_copy(half, b, 0, lax.rem(x + 1, nx)).wait_recv()

                turn(b, half * middle, (half + 1) * middle)

                @pl.loop(half * middle, (half + 1) * middle, unroll=2)
                def _(g):
                    forward(b, g, False)

    for entry in pass_second:
        pass_on(entry)

    earlier(0)

    ahead, behind = second_leg[0::2], second_leg[1::2]
    ahead += behind[reach - 1 :]
    behind = behind[: reach - 1]
    half = reach // 2
    pieces = [
        (ahead[:half], reach + 1, reach + 1 + half),
        (behind[:half], nz - reach - half, nz - reach),
        (ahead[half:], reach + 1 + half, 2 * reach + 1),
        (behind[half:], 2 * reach + 1, nz - reach - half),
    ]
    for arrivals, begin, end in pieces:
        for c in arrivals:
            c.wait_recv()
        if end > begin:
            for c in to_columns(begin, end):
                c.start()

    earlier(1)

    pltpu.make_async_copy(rows.at[1:nx], rows.at[1:nx], rx_recv).wait()

    for d in range(nx):
        part_rows = nz * 2 * groups
        rows32[d * part_rows : (d + 1) * part_rows, :] = rows[d].astype(F32).reshape(part_rows, HEAD_DIM)
    for part in range(2):
        for g in range(groups):
            cols = slice(g * HEAD_DIM, (g + 1) * HEAD_DIM)
            block = rows32[pl.ds(part * groups + g, key_count, stride=2 * groups), :]
            kv[last, part, :, cols] = block.astype(BF16)
            kvt[last, part, cols, :] = block.T.astype(BF16)

    def x_copy(g, d):
        return remote(
            xsend.at[g, d], xrecv.at[g, nx - d], x_send, x_recv, at_x(d)
        )

    @pl.loop(0, groups, unroll=groups)
    def _(g):
        cols = pl.ds(pl.multiple_of(g * HEAD_DIM, HEAD_DIM), HEAD_DIM)
        keys = kv[last, 0, :, cols]
        values = kv[last, 1, :, cols]
        for t in range(tiles):
            at = slice(t * TILE, (t + 1) * TILE)
            s = dot(keys, qt_s[g * tiles + t])
            before = stat[g, 0:1, at]
            top = jnp.maximum(jnp.max(s, axis=0, keepdims=True), before)
            e = jnp.exp2((s - top) * fold)
            old = jnp.exp2((before - top) * fold)
            inverse = 1.0 / (old * stat[g, 1:2, at] + jnp.sum(e, axis=0, keepdims=True))
            dp = dot(values, gt_s[g * tiles + t])
            p = e * inverse
            mean = old * inverse * stat[g, 2:3, at] + jnp.sum(p * dp, axis=0, keepdims=True)
            pp_s[g, :, at] = p.astype(BF16)
            dsp_s[g, :, at] = (p * (dp - mean)).astype(BF16)
            stat[g, 0:1, at] = top
            stat[g, 1:2, at] = inverse
            stat[g, 2:3, at] = mean
            stat[g, 3:4, at] = old * inverse
        src = pl.ds(pl.multiple_of(g * wide, wide), wide)
        both = dot(dsp_s[g], q_s[src, :]) * scale, dot(pp_s[g], g_s[src, :])
        for part in range(2):
            xown[g, part] = both[part][:nz]
            for d in range(1, nx):
                xsend[g, d, part] = both[part][d * nz : (d + 1) * nz].astype(BF16)
        for d in range(1, nx):
            x_copy(g, d).start()

    def c_copy(b, g, slot, to):
        return remote(csend.at[b, g], crecv.at[slot, g], c_send.at[b, g], c_recv.at[slot, g], {"fsdp": to})

    @pl.loop(0, groups, unroll=groups)
    def _(g):
        both = backward(x, g, True)
        for part in range(2):
            cown[g, part] = both[part]

    def earlier_backward(n):
        edge = x == nx - 1
        b = lax.rem(n + edge.astype(jnp.int32), nx - 1)
        short = edge & (b == 0)
        more = jnp.logical_not(edge) & ((b > 0) | (x < nx - 2))
        slot = jnp.where(short, nx - 1, b)
        to = jnp.where(short, 0, x - 1)

        @pl.loop(0, groups // 2)
        def _(pair):
            for k in range(2):
                both = backward(b, 2 * pair + k, False)
                for part in range(2):
                    cterm[k, part] = both[part]
            for k in range(2):
                g = 2 * pair + k

                @pl.when(more)
                def _(g=g, k=k):
                    c_copy(b, g, b, to).wait_recv()
                    for part in range(2):
                        cterm[k, part] += crecv[b, g, part].astype(F32)

                for part in range(2):
                    csend[b, g, part] = cterm[k, part].astype(BF16)
                c_copy(b, g, slot, to).start()

    pltpu.make_async_copy(xrecv.at[:, 1:nx], xrecv.at[:, 1:nx], x_recv).wait()
    for g in range(groups):
        for part in range(2):
            total = xown[g, part]
            for d in range(1, nx):
                total += xrecv[g, d, part].astype(F32)
            zf[pl.ds(part * groups + g, nz, stride=2 * groups), :] = total
    zsend[...] = zf[...].reshape(nz, 2 * groups, HEAD_DIM).astype(BF16)

    def z_copy(s):
        return remote(zsend.at[s], zrecv.at[nz - s], z_send, z_recv, at_z(s))

    for s in sorted(range(1, nz), key=lambda s: min(s, nz - s), reverse=True):
        z_copy(s).start()

    @pl.loop(0, jnp.minimum(x, 1))
    def _(n):
        earlier_backward(n)

    @pl.loop(0, groups)
    def _(g):
        cols = pl.ds(pl.multiple_of(g * HEAD_DIM, HEAD_DIM), HEAD_DIM)
        values_t = kvt[last, 1, cols, :]
        flush(
            lambda at: o_s[g, :, at] * stat[g, 3:4, at] + dot(values_t, pp_s[g, :, at]),
            out,
            g,
        )

    @pl.loop(1, x)
    def _(n):
        earlier_backward(n)

    @pl.loop(0, groups)
    def _(g):
        flush(lambda at: dq_s[g, :, at] * scale, query_grad, g)

    def collect(slot):
        for g in range(groups):
            c_copy(0, g, slot, lax.rem(x + 1, nx)).wait_recv()
            for part in range(2):
                cown[g, part] += crecv[slot, g, part].astype(F32)

    @pl.when((x < nx - 1) & ((x > 0) | (x < nx - 2)))
    def _():
        collect(x)

    @pl.when(x == 0)
    def _():
        collect(nx - 1)

    for part, ref in enumerate((comp_k_grad, comp_v_grad)):
        for g in range(groups):
            ref[0, 0, :, g * HEAD_DIM : (g + 1) * HEAD_DIM] = cown[g, part]

    for entry in own_sends + pass_first + pass_second:

        @pl.when(x == entry[0])
        def _(entry=entry):
            kv_copy(*entry[1:]).wait_send()

    sent = rows.at[0, 0 : 2 * reach]
    pltpu.make_async_copy(sent, sent, r1_send).wait()
    sent = rows.at[0, 0 : 2 * reach - 1]
    pltpu.make_async_copy(sent, sent, r2_send).wait()
    pltpu.make_async_copy(rows.at[1:nx], rows.at[1:nx], rx_send).wait()
    pltpu.make_async_copy(xsend.at[:, 1:nx], xsend.at[:, 1:nx], x_send).wait()
    pltpu.make_async_copy(zsend.at[1:nz], zsend.at[1:nz], z_send).wait()

    @pl.loop(0, x)
    def _(b):
        for g in range(groups):
            c_copy(b, g, 0, lax.rem(x + 1, nx)).wait_send()

    pltpu.make_async_copy(zrecv.at[1:nz], zrecv.at[1:nz], z_recv).wait()
    total = zf[: 2 * groups, :]
    for s in range(1, nz):
        total += zrecv[s].astype(F32)
    for k, ref in enumerate((prompt_k_grad, prompt_v_grad)):
        for g in range(groups):
            ref[0, :, g * HEAD_DIM : (g + 1) * HEAD_DIM] = total[k * groups + g : k * groups + g + 1, :]


def hand_on(*refs):
    n = len(refs) // 2
    sem = refs[-1]
    copies = [pltpu.make_async_copy(refs[k], refs[n + k], sem.at[k]) for k in range(n)]
    for c in copies:
        c.start()
    for c in copies:
        c.wait()


def solution(mesh):
    nz, nx = mesh.shape["sample"], mesh.shape["fsdp"]

    def shards(queries, comp_k, comp_v, prompt_k, prompt_v, output_grad, lengths):
        count, width = queries.shape[2:]
        kv_width = comp_k.shape[3]
        groups = kv_width // HEAD_DIM
        heads = width // HEAD_DIM
        wide = heads // groups * count
        key_count = nz * nx
        reach = nz // 4
        blocks = nx + 1
        anywhere = pl.BlockSpec(memory_space=pl.ANY)
        vmem = pl.BlockSpec(memory_space=pltpu.VMEM)
        smem = pl.BlockSpec(memory_space=pltpu.SMEM)
        dma = pltpu.SemaphoreType.DMA
        one = jax.ShapeDtypeStruct
        results = pl.pallas_call(
            functools.partial(kernel, nz, nx),
            out_shape=(
                pltpu.VMEM(queries.shape, BF16),
                pltpu.VMEM(queries.shape, BF16),
                pltpu.VMEM(comp_k.shape, F32),
                pltpu.VMEM(comp_k.shape, F32),
                pltpu.VMEM(prompt_k.shape, F32),
                pltpu.VMEM(prompt_k.shape, F32),
            ),
            in_specs=[anywhere] * 6 + [smem],
            out_specs=(vmem,) * 6,
            scratch_shapes=[
                pltpu.VMEM((heads * count, HEAD_DIM), BF16),
                pltpu.VMEM((heads * count, HEAD_DIM), BF16),
                pltpu.VMEM((heads * count // TILE, HEAD_DIM, TILE), BF16),
                pltpu.VMEM((heads * count // TILE, HEAD_DIM, TILE), BF16),
                pltpu.VMEM((blocks, 2, count, kv_width), BF16),
                pltpu.VMEM((blocks, 2, kv_width, count), BF16),
                pltpu.VMEM((nx, nz, 2 * groups, HEAD_DIM), BF16),
                pltpu.VMEM((key_count * 2 * groups, HEAD_DIM), F32),
                pltpu.VMEM((groups * nx, count, wide), F32),
                pltpu.VMEM((groups * nx, count, wide), F32),
                pltpu.VMEM((groups, HEAD_DIM, wide), F32),
                pltpu.VMEM((groups, HEAD_DIM, wide), F32),
                pltpu.VMEM((groups, 8, wide), F32),
                pltpu.VMEM((groups * nx, 1, wide), F32),
                pltpu.VMEM((count, wide), BF16),
                pltpu.VMEM((count, wide), BF16),
                pltpu.VMEM((groups, key_count, wide), BF16),
                pltpu.VMEM((groups, key_count, wide), BF16),
                pltpu.VMEM((nx, groups, 2, count, HEAD_DIM), BF16),
                pltpu.VMEM((nx, groups, 2, count, HEAD_DIM), BF16),
                pltpu.VMEM((groups, 2, count, HEAD_DIM), F32),
                pltpu.VMEM((2, 2, count, HEAD_DIM), F32),
                pltpu.VMEM((groups, nx, 2, nz, HEAD_DIM), BF16),
                pltpu.VMEM((groups, 2, nz, HEAD_DIM), F32),
                pltpu.VMEM((groups, nx, 2, nz, HEAD_DIM), BF16),
                pltpu.VMEM((nz * 2 * groups, HEAD_DIM), F32),
                pltpu.VMEM((nz, 2 * groups, HEAD_DIM), BF16),
                pltpu.VMEM((nz, 2 * groups, HEAD_DIM), BF16),
                pltpu.VMEM((2 * groups, HEAD_DIM), F32),
                pltpu.VMEM((2, *prompt_k.shape), BF16),
                dma((2, groups)),
                dma((2,)),
                dma((2,)),
                dma,
                dma((2 * reach,)),
                dma,
                dma((2, reach)),
                dma,
                dma,
                dma((2, 3)),
                dma((2, nx)),
                dma,
                dma,
                dma,
                dma,
                dma((nx, groups)),
                dma((nx, groups)),
            ],
            compiler_params=pltpu.CompilerParams(
                collective_id=0, has_side_effects=True, vmem_limit_bytes=58 * 2**20
            ),
            name="attend",
        )(queries, comp_k, comp_v, prompt_k, prompt_v, output_grad, lengths)
        n = len(results)
        return pl.pallas_call(
            hand_on,
            out_shape=tuple(one(r.shape, r.dtype) for r in results),
            in_specs=[vmem] * n,
            out_specs=(anywhere,) * n,
            scratch_shapes=[dma((n,))],
            compiler_params=pltpu.CompilerParams(vmem_limit_bytes=2**20),
            name="hand_on",
        )(*(pltpu.with_memory_space_constraint(r, pltpu.VMEM) for r in results))

    rows = P(("groups", "prompt"), "sample", "fsdp", None)
    prompt_rows = P(("groups", "prompt"), ("sample", "fsdp"), None)
    return jax.shard_map(
        shards,
        mesh=mesh,
        in_specs=(rows, rows, rows, prompt_rows, prompt_rows, rows, P(("groups", "prompt"), "sample")),
        out_specs=(rows, rows, rows, rows, prompt_rows, prompt_rows),
        check_vma=False,
    )
```
